32 devices in a mesh: gx: 4 (over y, x), gy: 4 (over z), gz: 2 (over core).
Axes of the slice: x: 2, y: 2, z: 4, core: 2. Of those that a mesh axis runs over, the one named last changes fastest.
Arguments:
- residual_in: float32 [2, 4, 64, 64, 256], P(None, None, 'gx', 'gy', 'gz'), may hold values from -15 to 15
- reaction: float32 [4, 64, 64, 256], P(None, 'gx', 'gy', 'gz'), may hold values from 0.5 to 2
- transport: float32 [4, 64, 64, 256], P(None, 'gx', 'gy', 'gz'), may hold values from 0.2 to 1
- congestion: float32 [4, 64, 64, 256], P(None, 'gx', 'gy', 'gz'), may hold values from 0.5 to 1.5
Outputs:
- newton_update: float32 [2, 4, 64, 64, 256], P(None, None, 'gx', 'gy', 'gz')
The draws below stay inside these ranges and needn't reach their ends.
All inputs are finite; a program needn't handle non-finite values.
Results may differ from the reference program's by a relative error of at most 0.0003.
Values sent between devices are 32-bit elements; how exact they have to be, the bound alone decides.
A program may use at most 128 MiB of HBM per device.

```python
import jax
import jax.numpy as jnp

LEVELS = 4
ITERS = 8
NX = 64
NY = 64
NZ = 256


def level_of(own_key, shape, cuts, low, top_value):
    factor_of = 1.0
    for dim, blocks in cuts:
        draws = jax.random.uniform(jax.random.fold_in(jax.random.fold_in(own_key, 6), dim), (blocks,), jnp.float32, low / len(cuts), top_value / len(cuts))
        factor_of = factor_of * jnp.repeat(jnp.exp(draws), shape[dim] // blocks).reshape((-1,) + (1,) * (len(shape) - 1 - dim))
    return factor_of


def normal_values(rng, extent, scale, bound, pieces=(), held_as=jnp.bfloat16):
    drawn = jax.random.normal(rng, extent, jnp.float32) * scale
    if len(pieces) > 0:
        drawn = level_of(rng, extent, pieces, -0.22, 0.18) * drawn
    return jnp.clip(drawn, min=-bound, max=bound).astype(held_as)


def setup_inputs(seed: int = 0) -> dict:
    seeds = jax.random.split(jax.random.key(seed), 5)
    return {
        "residual_in": normal_values(seeds[0], (2, LEVELS, NX, NY, NZ), 3.0, 15.0, ((2, 4), (3, 4), (4, 2)), jnp.float32),
        "reaction": jnp.clip(0.5 + 1.5 * jax.random.uniform(seeds[1], (LEVELS, NX, NY, NZ), jnp.float32) ** level_of(seeds[1], (LEVELS, NX, NY, NZ), ((1, 4), (2, 4), (3, 2)), -0.2, 0.2), 0.5, 2.0),
        "transport": jnp.clip(0.2 + 0.8 * jax.random.uniform(seeds[2], (LEVELS, NX, NY, NZ), jnp.float32) ** level_of(seeds[2], (LEVELS, NX, NY, NZ), ((1, 4), (2, 4), (3, 2)), -0.2, 0.2), 0.2, 1.0),
        "congestion": jnp.clip(0.5 + 1.0 * jax.random.uniform(seeds[3], (LEVELS, NX, NY, NZ), jnp.float32) ** level_of(seeds[3], (LEVELS, NX, NY, NZ), ((1, 4), (2, 4), (3, 2)), -0.2, 0.2), 0.5, 1.5),
    }


time_rate = 1.0

def minus_laplace(field):
    padded = jnp.pad(field, ((0, 0), (0, 0), (1, 1), (1, 1), (1, 1)))
    center = padded[:, :, 1:-1, 1:-1, 1:-1]
    beside = padded[:, :, 2:, 1:-1, 1:-1] + padded[:, :, :-2, 1:-1, 1:-1]
    beside = beside + padded[:, :, 1:-1, 2:, 1:-1] + padded[:, :, 1:-1, :-2, 1:-1]
    beside = beside + padded[:, :, 1:-1, 1:-1, 2:] + padded[:, :, 1:-1, 1:-1, :-2]
    return 6.0 * center - beside

def jacobian(vector, lapped, reaction, transport, congestion):
    value_part, density_part = (vector[0], vector[1])
    later = jnp.concatenate([value_part[1:], jnp.zeros_like(value_part[:1])], 0)
    earlier = jnp.concatenate([jnp.zeros_like(density_part[:1]), density_part[:-1]], 0)
    first = time_rate * (value_part - later) + lapped[0] + reaction * value_part - congestion * density_part
    second = time_rate * (density_part - earlier) + lapped[1] + reaction * density_part - transport * lapped[0]
    return jnp.stack([first, second], 0)

def precondition(vector, reaction, transport):
    levels = vector.shape[1]
    diag = time_rate + 6.0 + reaction
    value_levels = [None] * levels
    carry = jnp.zeros_like(vector[0, 0])
    for level in range(levels - 1, -1, -1):
        carry = (vector[0, level] + time_rate * carry) / diag[level]
        value_levels[level] = carry
    density_levels = []
    carry = jnp.zeros_like(vector[1, 0])
    for level in range(levels):
        carry = (vector[1, level] + time_rate * carry + 6.0 * transport[level] * value_levels[level]) / diag[level]
        density_levels.append(carry)
    return jnp.stack([jnp.stack(value_levels, 0), jnp.stack(density_levels, 0)], 0)

def least_squares(columns, beta, steps):
    rotations = []
    target = [beta] + [jnp.float32(0.0)] * steps
    upper = []
    for column_index in range(steps):
        column = list(columns[column_index])
        for place, (cosine, sine) in enumerate(rotations):
            upper_entry = cosine * column[place] + sine * column[place + 1]
            lower_entry = -sine * column[place] + cosine * column[place + 1]
            column[place], column[place + 1] = (upper_entry, lower_entry)
        radius = jnp.sqrt(column[column_index] ** 2 + column[column_index + 1] ** 2)
        cosine = column[column_index] / radius
        sine = column[column_index + 1] / radius
        column[column_index] = radius
        rotations.append((cosine, sine))
        target[column_index], target[column_index + 1] = (cosine * target[column_index], -sine * target[column_index])
        upper.append(column[:column_index + 1])
    solved = [None] * steps
    for row_index in range(steps - 1, -1, -1):
        accum = target[row_index]
        for later_index in range(row_index + 1, steps):
            accum = accum - upper[later_index][row_index] * solved[later_index]
        solved[row_index] = accum / upper[row_index][row_index]
    return solved

def reference(residual_in, reaction, transport, congestion):
    beta = jnp.sqrt(jnp.sum(residual_in * residual_in))
    basis = [residual_in / beta]
    columns = []
    for column_index in range(ITERS):
        search = precondition(basis[column_index], reaction, transport)
        image = jacobian(search, minus_laplace(search), reaction, transport, congestion)
        coeffs = [jnp.sum(vector * image) for vector in basis]
        for coeff, vector in zip(coeffs, basis):
            image = image - coeff * vector
        height = jnp.sqrt(jnp.sum(image * image))
        basis.append(image / height)
        columns.append(coeffs + [height])
    solved = least_squares(columns, beta, ITERS)
    update = jnp.zeros_like(residual_in)
    for column_index in range(ITERS):
        update = update + solved[column_index] * precondition(basis[column_index], reaction, transport)
    return update
```

```python
import functools

import jax
import jax.numpy as jnp
from jax import lax
from jax.experimental import pallas as pl
from jax.experimental.pallas import tpu as pltpu
from jax.sharding import PartitionSpec as P

ITERS = 8
AXES = ("gx", "gy", "gz")
time_rate = 1.0
SCALE = 2.5
BACK = 1.0
PIVOT = 2.5e-3
PLANES = 4
PAD = 8
FIRST_BACK = 2
GROUP = 3
SPAN = 2
STARTS = ("x0", "y0", "gx", "gy")
CHANNELS = {
    "x": (8, 2, ITERS),
    "y": (24, 2, 4),
    "c": (32, 4, 4),
    ("z", 0): (48, 2, 2),
    ("z", 1): (52, 2, 4),
    ("z", 2): (60, 2, 2),
}


def gram_row(row, column):
    return column * (ITERS + 1) + row


def least_squares(columns, beta, steps):
    zero = jnp.zeros_like(beta)
    rotations = []
    target = [beta] + [zero] * steps
    upper = []
    for column_index in range(steps):
        column = list(columns[column_index])
        for place, (cosine, sine) in enumerate(rotations):
            upper_entry = cosine * column[place] + sine * column[place + 1]
            lower_entry = -sine * column[place] + cosine * column[place + 1]
            column[place], column[place + 1] = (upper_entry, lower_entry)
        radius = jnp.sqrt(column[column_index] ** 2 + column[column_index + 1] ** 2)
        inverse = 1.0 / radius
        cosine = column[column_index] * inverse
        sine = column[column_index + 1] * inverse
        column[column_index] = inverse
        rotations.append((cosine, sine))
        target[column_index], target[column_index + 1] = (
            cosine * target[column_index],
            -sine * target[column_index],
        )
        upper.append(column[: column_index + 1])
    solved = [None] * steps
    for row_index in range(steps - 1, -1, -1):
        accum = target[row_index]
        for later_index in range(steps - 1, row_index, -1):
            accum = accum - upper[later_index][row_index] * solved[later_index]
        solved[row_index] = accum * upper[row_index][row_index]
    return solved


def gram_solve(gram, steps):
    size = steps + 1
    work = {(i, j): gram(i, j) for j in range(size) for i in range(j + 1)}
    factor = {}
    worst = None
    for i in range(size):
        ratio = work[i, i] / gram(i, i)
        worst = ratio if worst is None else jnp.where(ratio > worst, worst, ratio)
        pivot = jnp.sqrt(work[i, i])
        inverse = 1.0 / pivot
        factor[i, i] = pivot
        for j in range(i + 1, size):
            factor[i, j] = work[i, j] * inverse
        for a in range(i + 1, size):
            for b in range(a, size):
                work[a, b] = work[a, b] - factor[i, a] * factor[i, b]
    columns = []
    for k in range(steps):
        column = []
        for i in range(k + 2):
            entry = -factor[i, k + 1] * (1.0 / SCALE)
            if i <= k:
                entry = entry + factor[i, k]
            if k >= FIRST_BACK and i <= k - 1:
                entry = entry - factor[i, k - 1] * (BACK / SCALE)
            column.append(entry)
        columns.append(column)
    return least_squares(columns, factor[0, 0], steps), worst


def kernel(
    levels, sizes, residual, reaction, transport, congestion, out, flag,
    basis, coef, inv, search, beside, xin, yin, yout, rows, cin, cout, zin, zout,
    ghost_x, ghost_y, ghost_inv, given, past, mixer, zsum, zside, gram, splat, gsend, gall,
    insem, ssem, rsem, gssem, grsem,
):
    fields = 2 * levels
    nx, ny, nz = residual.shape[1:]
    total = sizes[0] * sizes[1] * sizes[2]
    index = [lax.axis_index(axis) for axis in AXES]
    me = (index[0] * sizes[1] + index[1]) * sizes[2] + index[2]
    lane = lax.broadcasted_iota(jnp.int32, (ny, nz), 1)
    plane = pl.ds(0, ny)
    next_lane = (lane + 1) & (nz - 1)
    ends_mask = jnp.logical_or(lane == 0, lane == nz - 1)
    own = pl.ds(PAD, ny)
    blank = jnp.zeros((ny, nz), jnp.float32)
    weight, couple = coef.at[1], coef.at[2]

    loads = [
        pltpu.make_async_copy(src, dst, insem.at[place])
        for place, (src, dst) in enumerate((
            (residual, basis.at[1, :, pl.ds(0, nx), pl.ds(0, ny)]), (reaction, coef.at[0]),
            (transport, coef.at[1]), (congestion, coef.at[2]),
        ))
    ]
    for load in loads:
        load.start()

    for buffer in (xin, yin, cin, zin, ghost_x, ghost_y):
        buffer[...] = jnp.zeros_like(buffer)
    for slot in range(2):
        edge = nx + 1 if slot else 0
        search[0, :, edge] = jnp.zeros_like(search[0, :, edge])
    beside[0] = jnp.zeros_like(beside[0])
    past[...] = jnp.zeros_like(past)
    basis[0] = jnp.zeros_like(basis[0])
    gram[...] = jnp.zeros_like(gram)

    def ident(other):
        return (other // (sizes[1] * sizes[2]), (other // sizes[2]) % sizes[1], other % sizes[2])

    barrier = pltpu.get_barrier_semaphore()

    def greet(step, carry):
        pl.semaphore_signal(
            barrier, inc=1, device_id=ident((me + step) % total),
            device_id_type=pl.DeviceIdType.MESH,
        )
        return carry

    lax.fori_loop(1, total, greet, 0)

    def reaches(shift):
        ok = None
        for axis, move in enumerate(shift):
            if move == 0:
                continue
            this = index[axis] < sizes[axis] - 1 if move > 0 else index[axis] > 0
            ok = this if ok is None else jnp.logical_and(ok, this)
        return ok

    def remote(src, dst, place, shift):
        return pltpu.make_async_remote_copy(
            src_ref=src, dst_ref=dst, send_sem=ssem, recv_sem=rsem.at[place],
            device_id=tuple(i + move for i, move in zip(index, shift)),
            device_id_type=pl.DeviceIdType.MESH,
        )

    def number(key):
        kind, rest = key[0], key[1:]
        if kind in STARTS:
            return 2 * STARTS.index(kind) + rest[0]
        base, width, cycle = CHANNELS[kind if kind != "z" else (kind, rest[1])]
        spot = 0
        for part in rest[2 if kind == "z" else 1 :]:
            spot = 2 * spot + part
        return base + lax.rem(rest[0], cycle) * width + spot

    def start(key, src, dst, shift, wanted=None):
        go = reaches(shift)

        @pl.when(go if wanted is None else jnp.logical_and(go, wanted))
        def _():
            remote(src, dst, number(key), shift).start()

    def arrive(key, dst, shift):
        @pl.when(reaches([-move for move in shift]))
        def _():
            remote(dst, dst, number(key), shift).wait_recv()

    def drain(key, src, shift, wanted=None):
        go = reaches(shift)

        @pl.when(go if wanted is None else jnp.logical_and(go, wanted))
        def _():
            remote(src, src, number(key), shift).wait_send()

    def along(axis, side):
        shift = [0, 0, 0]
        shift[axis] = 1 if side == 0 else -1
        return shift

    def x_plane(near, side):
        return nx - near if side == 0 else 1 + near

    def send_x(k, wanted=None):
        for side in range(2):
            start(("x", k, side), search.at[k, :, x_plane(1, side), own],
                  xin.at[k, side], along(0, side), wanted)

    def send_y(k, wanted=None):
        for side in range(2):
            start(("y", k, side), yout.at[k, side], yin.at[k, side], along(1, side), wanted)

    def send_c(k, wanted=None):
        for cx in range(2):
            for cy in range(2):
                shift = [1 - 2 * cx, 1 - 2 * cy, 0]
                start(("c", k, cx, cy), cout.at[k, cx, cy], cin.at[k, cx, cy], shift, wanted)

    def send_z(k, kind, packs, wanted=None):
        for side in range(2):
            zout[k, kind, side] = packs[side]
            start(("z", k, kind, side), zout.at[k, kind, side], zin.at[k, kind, side],
                  along(2, side), wanted)

    def take_x(k):
        for side in range(2):
            arrive(("x", k, side), xin.at[k, side], along(0, side))

    def take_y(k):
        for side in range(2):
            arrive(("y", k, side), yin.at[k, side], along(1, side))

    def take_c(k):
        for cx in range(2):
            for cy in range(2):
                arrive(("c", k, cx, cy), cin.at[k, cx, cy], [1 - 2 * cx, 1 - 2 * cy, 0])

    def take_z(k, kind):
        for side in range(2):
            arrive(("z", k, kind, side), zin.at[k, kind, side], along(2, side))

    def precondition(scale, mass, vector):
        value, density = [None] * levels, [None] * levels
        carry = None
        for t in range(levels - 1, -1, -1):
            carry = vector[t] if carry is None else vector[t] + carry
            carry = carry * scale(t)
            value[t] = carry
        carry = None
        for t in range(levels):
            push = vector[levels + t] + (6.0 * mass(t)) * value[t]
            carry = push if carry is None else push + carry
            carry = carry * scale(t)
            density[t] = carry
        return value + density

    def mix(founds):
        blends = []
        for odd in range(2):
            whole = jnp.concatenate([found[f] for found in founds for f in range(odd, fields, 2)], 0)
            high = whole.astype(jnp.bfloat16)
            low = (whole - high.astype(jnp.float32)).astype(jnp.bfloat16)
            blends.append(jnp.dot(
                jnp.concatenate([high, low], 1), mixer[odd], preferred_element_type=jnp.float32
            ))
        mixed = []
        for place in range(len(founds)):
            parts = []
            for f in range(fields):
                row = (place * (fields // 2) + f // 2) * ny
                parts.append((blends[f % 2][row : row + ny, :nz], blends[f % 2][row : row + ny, nz:]))
            mixed.append(parts)
        return mixed

    def pack(packs, base, mixed):
        high, low = packs
        for f in range(fields):
            place = base + f
            high = jnp.where(lane == place, mixed[f][1], high)
            low = jnp.where(next_lane == place, mixed[f][1], low)
        return high, low

    def advance(k, kind, base, center, low, high, below, above, beyond, mass, pull, prior):
        zlow, zhigh = zin.at[k, kind, 0], zin.at[k, kind, 1]

        def around(f):
            place = base + f
            edge = jnp.where(lane == place, zlow[...], zhigh[...])
            edge = jnp.where(ends_mask, pltpu.roll(edge, (nz - place) & (nz - 1), 1), 0.0)
            return ((below(f) + above(f)) + (low(f) + high(f))) + (beyond(f) + edge)

        found = [None] * fields
        for t in range(levels):
            value = around(t)
            density = around(levels + t) - mass(t) * value
            value = value + pull(t) * center(levels + t)
            for f, item in ((t, value), (levels + t, density)):
                found[f] = SCALE * item - BACK * prior(f)
        return found

    def publish(k, x, found, fixed):
        for f in range(fields):
            search[k, f, x + 1, own] = found[f]
            for side, (edge, near) in enumerate(((0, ny - 2), (ny - 1, 1))):
                rows[k, side, f, pl.ds(x, 1), :] = found[f][edge : edge + 1, :]
                yout[k, side, f, pl.ds(x, 1), :] = found[f][near : near + 1, :]
            if fixed is not None:
                for cy in range(2):
                    edge = ny - 1 if cy == 0 else 0
                    cout[k, fixed, cy, f : f + 1, :] = found[f][edge : edge + 1, :]

    def own_planes(k, planes, packs):
        before = k * lax.div(lax.div(k, 2) + ITERS - 2, ITERS - 1)
        founds = []
        for x, fixed in planes:
            vector = advance(
                k, 0, x * fields,
                lambda f: search[k, f, x + 1, own],
                lambda f: search[k, f, x + 1, pl.ds(PAD - 1, ny)],
                lambda f: search[k, f, x + 1, pl.ds(PAD + 1, ny)],
                lambda f: search[k, f, x, own],
                lambda f: search[k, f, x + 2, own],
                lambda f: zsum[lax.rem(k, 2), f, x + 1],
                lambda t: weight[t, x],
                lambda t: couple[t, x],
                lambda f: basis[before, f, x, plane],
            )
            for f in range(fields):
                basis[k + 2, f, x, plane] = vector[f]
            founds.append(
                precondition(lambda t: inv[t, x], lambda t: weight[t, x], vector)
            )
        return spread(k + 1, planes, founds, packs)

    def spread(k, planes, founds, packs):
        for (x, fixed), found, mixed in zip(planes, founds, mix(founds)):
            packs = pack(packs, x * fields, mixed)
            publish(k, x, found, fixed)
            for f in range(fields):
                zsum[lax.rem(k, 2), f, x + 1] = mixed[f][0]
        return packs

    def scatter(k, side, get):
        row = PAD - 1 if side == 0 else PAD + ny
        for f in range(fields):
            found = get(f)
            for x in range(nx):
                search[k, f, x + 1, row : row + 1, :] = found[x : x + 1, :]

    def aside(k, side, found, packs):
        mixed = mix([found])[0]
        for f in range(fields):
            zside[lax.rem(k, 2), side, f] = mixed[f][0]
        return pack(packs, side * fields, mixed)

    def across(k, side, edge, found, packs):
        mixed = mix([found])[0]
        for f in range(fields):
            zsum[lax.rem(k, 2), f, edge] = mixed[f][0]
        return pack(packs, side * fields, mixed)

    def y_given():
        packs = (blank, blank)
        for side in range(2):
            arrive(("y0", side), beside.at[0, side, :, own], along(1, side))
        for side in range(2):
            found = [beside[0, side, f, own] for f in range(fields)]
            scatter(0, side, lambda f: found[f])
            packs = aside(0, side, found, packs)
        send_z(0, 1, packs)
        for axis, ghost in enumerate((ghost_x, ghost_y)):
            for side in range(2):
                arrive(("gx" if axis == 0 else "gy", side), ghost.at[side], along(axis, side))
                there = index[axis] > 0 if side == 0 else index[axis] < sizes[axis] - 1
                for t in range(levels):
                    ghost_inv[axis, side, t] = jnp.where(
                        there, 1.0 / (time_rate + 6.0 + ghost[side, 0, t]), 0.0
                    )

    def y_ghosts(k):
        packs = (blank, blank)
        j = k - 1
        take_y(j)
        take_c(j)
        take_z(j, 1)
        for side in range(2):
            for f in range(fields):
                beside[j, side, f, PAD - 1 : PAD, :] = cin[j, 0, side, f : f + 1, :]
                beside[j, side, f, PAD + nx : PAD + nx + 1, :] = cin[j, 1, side, f : f + 1, :]
            vector = advance(
                j, 1, side * fields,
                lambda f: beside[j, side, f, own],
                lambda f: beside[j, side, f, pl.ds(PAD - 1, nx)],
                lambda f: beside[j, side, f, pl.ds(PAD + 1, nx)],
                lambda f: yin[j, side, f],
                lambda f: rows[j, side, f],
                lambda f: zside[lax.rem(j, 2), side, f],
                lambda t: ghost_y[side, 1, t],
                lambda t: ghost_y[side, 2, t],
                lambda f: past[lax.rem(k, 2), 1, side, f],
            )
            for f in range(fields):
                past[lax.rem(k, 2), 1, side, f] = vector[f]
            found = precondition(
                lambda t: ghost_inv[1, side, t], lambda t: ghost_y[side, 1, t], vector
            )
            for f in range(fields):
                beside[k, side, f, own] = found[f]
            scatter(k, side, lambda f: found[f])
            packs = aside(k, side, found, packs)
        send_z(k, 1, packs, k < ITERS - 1)

    def x_given():
        packs = (blank, blank)
        for side in range(2):
            edge = nx + 1 if side else 0
            arrive(("x0", side), search.at[0, :, edge, own], along(0, side))
            found = [search[0, f, edge, own] for f in range(fields)]
            packs = across(0, side, edge, found, packs)
        send_z(0, 2, packs)

    def x_ghosts(k):
        packs = (blank, blank)
        j = k - 1
        take_x(j)
        take_z(j, 2)
        for side in range(2):
            edge, inner = (0, 1) if side == 0 else (nx + 1, nx)
            for f in range(fields):
                search[j, f, edge, PAD - 1 : PAD, :] = cin[j, side, 0, f : f + 1, :]
                search[j, f, edge, PAD + ny : PAD + ny + 1, :] = cin[j, side, 1, f : f + 1, :]
            vector = advance(
                j, 2, side * fields,
                lambda f: search[j, f, edge, own],
                lambda f: search[j, f, edge, pl.ds(PAD - 1, ny)],
                lambda f: search[j, f, edge, pl.ds(PAD + 1, ny)],
                lambda f: xin[j, side, f],
                lambda f: search[j, f, inner, own],
                lambda f: zsum[lax.rem(j, 2), f, edge],
                lambda t: ghost_x[side, 1, t],
                lambda t: ghost_x[side, 2, t],
                lambda f: past[lax.rem(k, 2), 0, side, f],
            )
            for f in range(fields):
                past[lax.rem(k, 2), 0, side, f] = vector[f]
            found = precondition(
                lambda t: ghost_inv[0, side, t], lambda t: ghost_x[side, 1, t], vector
            )
            for f in range(fields):
                search[k, f, edge, own] = found[f]
            packs = across(k, side, edge, found, packs)
        send_z(k, 2, packs, k < ITERS - 1)

    def dots(k):
        def group(g, carry):
            def step(place, accs):
                sums = [[] for _ in range(GROUP)]
                for x in range(SPAN):
                    x = place * SPAN + x
                    mine = [basis[k + 1, f, x, plane] for f in range(fields)]
                    for i in range(GROUP):
                        terms = [mine[f] * basis[g * GROUP + i + 1, f, x, plane] for f in range(fields)]
                        while len(terms) > 1:
                            terms = [a + b for a, b in zip(terms[::2], terms[1::2])]
                        sums[i].append(terms[0])
                return tuple(acc + sum(more) for acc, more in zip(accs, sums))

            accs = lax.fori_loop(0, nx // SPAN, step, (blank,) * GROUP)
            for i in range(GROUP):
                row = gram_row(g * GROUP + i, k)
                gram[pl.ds(row, 1), :] = jnp.sum(accs[i], axis=0, keepdims=True)
            return carry

        lax.fori_loop(0, lax.div(k, GROUP) + 1, group, 0)

    for load in loads:
        load.wait()

    def invert(x, carry):
        for t in range(levels):
            inv[t, x] = 1.0 / (time_rate + 6.0 + coef[0, t, x])
            for which in range(3):
                item = coef[which, t, x]
                given[0, which, t, pl.ds(x, 1), :] = item[ny - 1 : ny, :]
                given[1, which, t, pl.ds(x, 1), :] = item[0:1, :]
        return carry

    lax.fori_loop(0, nx, invert, 0)
    def first(planes, packs):
        founds = [
            precondition(
                lambda t: inv[t, x], lambda t: weight[t, x],
                [basis[1, f, x, plane] for f in range(fields)],
            )
            for x, _ in planes
        ]
        return spread(0, planes, founds, packs)

    def sweep(body, packs, low):
        return lax.fori_loop(
            0, (nx - 2 * low) // PLANES,
            lambda step, packs: body(
                [(low + step * PLANES + place, None) for place in range(PLANES)], packs
            ),
            packs,
        )

    pl.semaphore_wait(barrier, total - 1)
    for side in range(2):
        start(("gx", side), coef.at[:, :, nx - 1 if side == 0 else 0], ghost_x.at[side],
              along(0, side))
    for side in range(2):
        start(("gy", side), given.at[side], ghost_y.at[side], along(1, side))
    from_lane = lax.broadcasted_iota(jnp.int32, (2 * nz, 2 * nz), 0) & (nz - 1)
    to_lane = lax.broadcasted_iota(jnp.int32, (2 * nz, 2 * nz), 1)
    for odd in range(2):
        beside_lane = jnp.logical_or(from_lane - to_lane == 1, to_lane - from_lane == 1)
        last_lane = jnp.logical_and((to_lane & 1) == odd, from_lane == nz - 1)
        first_lane = jnp.logical_and((to_lane & 1) != odd, from_lane == 0)
        taken = jnp.where(
            to_lane < nz, beside_lane.astype(jnp.int32),
            jnp.logical_or(last_lane, first_lane).astype(jnp.int32),
        )
        mixer[odd] = taken.astype(jnp.float32).astype(jnp.bfloat16)
    ends = [(0, 1), (nx - 1, 0)]
    packs = first(ends, (blank, blank))
    packs = first([(1, None), (nx - 2, None)], packs)
    packs = sweep(first, packs, 2)
    for side in range(2):
        start(("x0", side), search.at[0, :, nx if side == 0 else 1, own],
              search.at[0, :, nx + 1 if side else 0, own], along(0, side))
    for side in range(2):
        start(("y0", side), rows.at[0, 1 - side], beside.at[0, side, :, own], along(1, side))
    send_z(0, 0, packs)
    send_c(0)
    send_x(0)
    send_y(0)
    dots(0)
    y_given()

    def iterate(k, carry):
        more = k < ITERS - 2

        @pl.when(k > 0)
        def _():
            y_ghosts(k)

        take_z(k, 0)
        body = functools.partial(own_planes, k)
        packs = body([(1, None), (nx - 2, None)], (blank, blank))
        send_x(k + 1, more)
        packs = sweep(body, packs, 2)

        @pl.when(k == 0)
        def _():
            x_given()

        @pl.when(k > 0)
        def _():
            x_ghosts(k)

        packs = body(ends, packs)
        send_z(k + 1, 0, packs, k < ITERS - 1)
        send_c(k + 1, more)
        send_y(k + 1, more)
        dots(k + 1)
        return carry

    lax.fori_loop(0, ITERS, iterate, 0)

    def settle(k, carry):
        more = k < ITERS - 1
        for side in range(2):
            drain(("x", k, side), xin.at[k, side], along(0, side), more)
            drain(("y", k, side), yin.at[k, side], along(1, side), more)
            for cy in range(2):
                drain(("c", k, side, cy), cin.at[k, side, cy], [1 - 2 * side, 1 - 2 * cy, 0], more)
            for kind in range(3):
                drain(("z", k, kind, side), zin.at[k, kind, side], along(2, side),
                      None if kind == 0 else more)
        return carry

    lax.fori_loop(0, ITERS, settle, 0)
    for side in range(2):
        drain(("x0", side), search.at[0, :, 0, own], along(0, side))
        drain(("y0", side), beside.at[0, side, :, own], along(1, side))
        drain(("gx", side), ghost_x.at[side], along(0, side))
        drain(("gy", side), ghost_y.at[side], along(1, side))

    local = jnp.sum(gram[...].T, axis=0, keepdims=True)
    gsend[...] = local
    gall[me] = local

    def spread(step, carry):
        pltpu.make_async_remote_copy(
            src_ref=gsend, dst_ref=gall.at[me], send_sem=gssem, recv_sem=grsem,
            device_id=ident((me + step) % total), device_id_type=pl.DeviceIdType.MESH,
        ).start()
        return carry

    lax.fori_loop(1, total, spread, 0)
    others = gall.at[pl.ds(0, total - 1)]
    pltpu.make_async_copy(others, others, grsem).wait()
    pltpu.make_async_copy(others, others, gssem).wait()
    whole = jnp.sum(gall[...], axis=0)
    splat[...] = jnp.broadcast_to(whole, splat.shape).T

    def entry(i, j):
        row = gram_row(i, j)
        return splat[row : row + 1, :]

    solved, worst = gram_solve(entry, ITERS)
    flag[...] = jnp.broadcast_to(worst, flag.shape)

    def combine(x, carry):
        for f in range(fields):
            item = solved[0] * search[0, f, x + 1, own]
            for k in range(1, ITERS):
                item = item + solved[k] * search[k, f, x + 1, own]
            out[f, x] = item
        return carry

    lax.fori_loop(0, nx, combine, 0)


def fused(sizes, residual, reaction, transport, congestion):
    levels, nx, ny, nz = reaction.shape
    fields = 2 * levels
    total = sizes[0] * sizes[1] * sizes[2]
    pairs = (ITERS + 1) ** 2
    assert (ITERS + 1) % GROUP == 0
    assert fields * nx <= nz and pairs <= nz and (nx - 4) % PLANES == 0 and nx == ny
    assert nz & (nz - 1) == 0
    f32 = jnp.float32
    hbm = pl.BlockSpec(memory_space=pl.ANY)
    vmem = pl.BlockSpec(memory_space=pltpu.VMEM)
    wide = ny + 3 * PAD
    copies = sum(width * cycle for _, width, cycle in CHANNELS.values()) + 2 * len(STARTS)
    out, flag = pl.pallas_call(
        functools.partial(kernel, levels, sizes),
        out_shape=(
            jax.ShapeDtypeStruct((fields, nx, ny, nz), f32),
            jax.ShapeDtypeStruct((8, nz), f32),
        ),
        in_specs=[hbm] * 4,
        out_specs=(vmem, vmem),
        scratch_shapes=[
            pltpu.VMEM((ITERS + 2, fields, nx + 1, ny + PAD, nz), f32),
            pltpu.VMEM((3, levels, nx, ny, nz), f32),
            pltpu.VMEM((levels, nx, ny, nz), f32),
            pltpu.VMEM((ITERS + 1, fields, nx + 2, wide, nz), f32),
            pltpu.VMEM((ITERS, 2, fields, wide, nz), f32),
            pltpu.VMEM((ITERS + 1, 2, fields, ny, nz), f32),
            pltpu.VMEM((ITERS + 1, 2, fields, nx, nz), f32),
            pltpu.VMEM((ITERS + 1, 2, fields, nx, nz), f32),
            pltpu.VMEM((ITERS + 1, 2, fields, nx, nz), f32),
            pltpu.VMEM((ITERS + 1, 2, 2, fields, nz), f32),
            pltpu.VMEM((ITERS + 1, 2, 2, fields, nz), f32),
            pltpu.VMEM((ITERS + 1, 3, 2, ny, nz), f32),
            pltpu.VMEM((ITERS + 1, 3, 2, ny, nz), f32),
            pltpu.VMEM((2, 3, levels, ny, nz), f32),
            pltpu.VMEM((2, 3, levels, nx, nz), f32),
            pltpu.VMEM((2, 2, levels, ny, nz), f32),
            pltpu.VMEM((2, 3, levels, nx, nz), f32),
            pltpu.VMEM((2, 2, 2, fields, ny, nz), f32),
            pltpu.VMEM((2, 2 * nz, 2 * nz), jnp.bfloat16),
            pltpu.VMEM((2, fields, nx + 2, ny, nz), f32),
            pltpu.VMEM((2, 2, fields, nx, nz), f32),
            pltpu.VMEM((nz, nz), f32),
            pltpu.VMEM((nz, nz), f32),
            pltpu.VMEM((1, nz), f32),
            pltpu.VMEM((total, 1, nz), f32),
            pltpu.SemaphoreType.DMA((4,)),
            pltpu.SemaphoreType.DMA,
            pltpu.SemaphoreType.DMA((copies,)),
            pltpu.SemaphoreType.DMA,
            pltpu.SemaphoreType.DMA,
        ],
        compiler_params=pltpu.CompilerParams(
            collective_id=0, has_side_effects=True, vmem_limit_bytes=60 * 1024 * 1024
        ),
        name="krylov",
    )(residual.reshape((fields, nx, ny, nz)), reaction, transport, congestion)
    return out.reshape(residual.shape), flag


def neighbours(field):
    total = 0.0
    for axis, dim in (("gx", 2), ("gy", 3), ("gz", 4)):
        count = lax.axis_size(axis)
        size = field.shape[dim]
        forward = [(i, i + 1) for i in range(count - 1)]
        backward = [(target, source) for source, target in forward]
        low = lax.ppermute(lax.slice_in_dim(field, size - 1, size, axis=dim), axis, forward)
        high = lax.ppermute(lax.slice_in_dim(field, 0, 1, axis=dim), axis, backward)
        below = jnp.concatenate([low, lax.slice_in_dim(field, 0, size - 1, axis=dim)], dim)
        above = jnp.concatenate([lax.slice_in_dim(field, 1, size, axis=dim), high], dim)
        total = total + below + above
    return total


def jacobian(vector, reaction, transport, congestion):
    lapped = 6.0 * vector - neighbours(vector)
    value_part, density_part = (vector[0], vector[1])
    later = jnp.concatenate([value_part[1:], jnp.zeros_like(value_part[:1])], 0)
    earlier = jnp.concatenate([jnp.zeros_like(density_part[:1]), density_part[:-1]], 0)
    first = (
        time_rate * (value_part - later)
        + lapped[0]
        + reaction * value_part
        - congestion * density_part
    )
    second = (
        time_rate * (density_part - earlier)
        + lapped[1]
        + reaction * density_part
        - transport * lapped[0]
    )
    return jnp.stack([first, second], 0)


def precondition(vector, reaction, transport):
    levels = vector.shape[1]
    diag = time_rate + 6.0 + reaction
    value_levels = [None] * levels
    carry = jnp.zeros_like(vector[0, 0])
    for level in range(levels - 1, -1, -1):
        carry = (vector[0, level] + time_rate * carry) / diag[level]
        value_levels[level] = carry
    density_levels = []
    carry = jnp.zeros_like(vector[1, 0])
    for level in range(levels):
        carry = (
            vector[1, level] + time_rate * carry + 6.0 * transport[level] * value_levels[level]
        ) / diag[level]
        density_levels.append(carry)
    return jnp.stack([jnp.stack(value_levels, 0), jnp.stack(density_levels, 0)], 0)


def arnoldi(residual, reaction, transport, congestion):
    dims = tuple(range(1, residual.ndim + 1))
    beta = jnp.sqrt(lax.psum(jnp.sum(residual * residual), AXES))
    basis = jnp.zeros((ITERS + 1,) + residual.shape, residual.dtype).at[0].set(residual / beta)
    heights = jnp.zeros((ITERS, ITERS + 1), residual.dtype)

    def step(c, state):
        basis, heights = state
        search = precondition(basis[c], reaction, transport)
        image = jacobian(search, reaction, transport, congestion)
        coeffs = lax.psum(jnp.sum(basis * image[None], axis=dims), AXES)
        image = image - jnp.sum(coeffs.reshape((-1,) + (1,) * residual.ndim) * basis, axis=0)
        height = jnp.sqrt(lax.psum(jnp.sum(image * image), AXES))
        basis = basis.at[c + 1].set(image / height)
        return basis, heights.at[c].set(coeffs.at[c + 1].set(height))

    basis, heights = lax.fori_loop(0, ITERS, step, (basis, heights))
    columns = [[heights[c, i] for i in range(c + 2)] for c in range(ITERS)]
    solved = least_squares(columns, beta, ITERS)
    mixed = sum(solved[c] * basis[c] for c in range(ITERS))
    return precondition(mixed, reaction, transport)


def body(sizes, residual_in, reaction, transport, congestion):
    update, flag = fused(sizes, residual_in, reaction, transport, congestion)
    return lax.cond(
        flag[0, 0] > PIVOT,
        lambda update, *rest: update,
        lambda update, *rest: arnoldi(*rest),
        update, residual_in, reaction, transport, congestion,
    )


def solution(mesh):
    placed = (
        P(None, None, "gx", "gy", "gz"),
        P(None, "gx", "gy", "gz"),
        P(None, "gx", "gy", "gz"),
        P(None, "gx", "gy", "gz"),
    )
    sizes = tuple(mesh.shape[axis] for axis in AXES)
    return jax.shard_map(
        functools.partial(body, sizes), mesh=mesh, in_specs=placed,
        out_specs=P(None, None, "gx", "gy", "gz"), check_vma=False,
    )
```

```python
import functools

import jax
import jax.numpy as jnp
from jax import lax
from jax.experimental import pallas as pl
from jax.experimental.pallas import tpu as pltpu
from jax.sharding import PartitionSpec as P

ITERS = 8
AXES = ("gx", "gy", "gz")
time_rate = 1.0
SCALE = 2.5
BACK = 1.0
PIVOT = 2.5e-3
PLANES = 4
PAD = 8
FIRST_BACK = 2
GROUP = 3
SPAN = 4
STARTS = ("x0", "y0", "gx", "gy")
CHANNELS = {
    "x": (8, 2, ITERS),
    "y": (24, 2, 4),
    "c": (32, 4, 4),
    ("z", 0): (48, 2, 2),
    ("z", 1): (52, 2, 4),
    ("z", 2): (60, 2, 2),
}


def gram_row(row, column):
    return column * (ITERS + 1) + row


def least_squares(columns, beta, steps):
    zero = jnp.zeros_like(beta)
    rotations = []
    target = [beta] + [zero] * steps
    upper = []
    for column_index in range(steps):
        column = list(columns[column_index])
        for place, (cosine, sine) in enumerate(rotations):
            upper_entry = cosine * column[place] + sine * column[place + 1]
            lower_entry = -sine * column[place] + cosine * column[place + 1]
            column[place], column[place + 1] = (upper_entry, lower_entry)
        radius = jnp.sqrt(column[column_index] ** 2 + column[column_index + 1] ** 2)
        inverse = 1.0 / radius
        cosine = column[column_index] * inverse
        sine = column[column_index + 1] * inverse
        column[column_index] = inverse
        rotations.append((cosine, sine))
        target[column_index], target[column_index + 1] = (
            cosine * target[column_index],
            -sine * target[column_index],
        )
        upper.append(column[: column_index + 1])
    solved = [None] * steps
    for row_index in range(steps - 1, -1, -1):
        accum = target[row_index]
        for later_index in range(steps - 1, row_index, -1):
            accum = accum - upper[later_index][row_index] * solved[later_index]
        solved[row_index] = accum * upper[row_index][row_index]
    return solved


def gram_solve(gram, steps):
    size = steps + 1
    work = {(i, j): gram(i, j) for j in range(size) for i in range(j + 1)}
    factor = {}
    worst = None
    for i in range(size):
        ratio = work[i, i] / gram(i, i)
        worst = ratio if worst is None else jnp.where(ratio > worst, worst, ratio)
        pivot = jnp.sqrt(work[i, i])
        inverse = 1.0 / pivot
        factor[i, i] = pivot
        for j in range(i + 1, size):
            factor[i, j] = work[i, j] * inverse
        for a in range(i + 1, size):
            for b in range(a, size):
                work[a, b] = work[a, b] - factor[i, a] * factor[i, b]
    columns = []
    for k in range(steps):
        column = []
        for i in range(k + 2):
            entry = -factor[i, k + 1] * (1.0 / SCALE)
            if i <= k:
                entry = entry + factor[i, k]
            if k >= FIRST_BACK and i <= k - 1:
                entry = entry - factor[i, k - 1] * (BACK / SCALE)
            column.append(entry)
        columns.append(column)
    return least_squares(columns, factor[0, 0], steps), worst


def kernel(
    levels, sizes, residual, reaction, transport, congestion, out, flag,
    basis, coef, inv, search, beside, xin, yin, yout, rows, cin, cout, zin, zout,
    ghost_x, ghost_y, ghost_inv, given, past, mixer, zsum, zside, gram, splat, gsend, gall,
    ready, insem, ssem, rsem, gssem, grsem, osem,
):
    fields = 2 * levels
    nx, ny, nz = residual.shape[1:]
    total = sizes[0] * sizes[1] * sizes[2]
    index = [lax.axis_index(axis) for axis in AXES]
    me = (index[0] * sizes[1] + index[1]) * sizes[2] + index[2]
    lane = lax.broadcasted_iota(jnp.int32, (ny, nz), 1)
    plane = pl.ds(0, ny)
    next_lane = (lane + 1) & (nz - 1)
    ends_mask = jnp.logical_or(lane == 0, lane == nz - 1)
    own = pl.ds(PAD, ny)
    blank = jnp.zeros((ny, nz), jnp.float32)
    weight, couple = coef.at[1], coef.at[2]

    loads = [
        pltpu.make_async_copy(src, dst, insem.at[place])
        for place, (src, dst) in enumerate((
            (residual, basis.at[1, :, pl.ds(0, nx), pl.ds(0, ny)]), (reaction, coef.at[0]),
            (transport, coef.at[1]), (congestion, coef.at[2]),
        ))
    ]
    for load in loads:
        load.start()

    for buffer in (xin, yin, cin, zin, ghost_x, ghost_y):
        buffer[...] = jnp.zeros_like(buffer)
    for slot in range(2):
        edge = nx + 1 if slot else 0
        search[0, :, edge] = jnp.zeros_like(search[0, :, edge])
    beside[0] = jnp.zeros_like(beside[0])
    past[...] = jnp.zeros_like(past)
    basis[0] = jnp.zeros_like(basis[0])
    gram[...] = jnp.zeros_like(gram)

    def ident(other):
        return (other // (sizes[1] * sizes[2]), (other // sizes[2]) % sizes[1], other % sizes[2])

    barrier = pltpu.get_barrier_semaphore()

    def greet(step, carry):
        pl.semaphore_signal(
            barrier, inc=1, device_id=ident((me + step) % total),
            device_id_type=pl.DeviceIdType.MESH,
        )
        return carry

    lax.fori_loop(1, total, greet, 0)

    def reaches(shift):
        ok = None
        for axis, move in enumerate(shift):
            if move == 0:
                continue
            this = index[axis] < sizes[axis] - 1 if move > 0 else index[axis] > 0
            ok = this if ok is None else jnp.logical_and(ok, this)
        return ok

    def remote(src, dst, place, shift):
        return pltpu.make_async_remote_copy(
            src_ref=src, dst_ref=dst, send_sem=ssem, recv_sem=rsem.at[place],
            device_id=tuple(i + move for i, move in zip(index, shift)),
            device_id_type=pl.DeviceIdType.MESH,
        )

    def number(key):
        kind, rest = key[0], key[1:]
        if kind in STARTS:
            return 2 * STARTS.index(kind) + rest[0]
        base, width, cycle = CHANNELS[kind if kind != "z" else (kind, rest[1])]
        spot = 0
        for part in rest[2 if kind == "z" else 1 :]:
            spot = 2 * spot + part
        return base + lax.rem(rest[0], cycle) * width + spot

    def start(key, src, dst, shift, wanted=None):
        go = reaches(shift)

        @pl.when(go if wanted is None else jnp.logical_and(go, wanted))
        def _():
            remote(src, dst, number(key), shift).start()

    def arrive(key, dst, shift):
        @pl.when(reaches([-move for move in shift]))
        def _():
            remote(dst, dst, number(key), shift).wait_recv()

    def drain(key, src, shift, wanted=None):
        go = reaches(shift)

        @pl.when(go if wanted is None else jnp.logical_and(go, wanted))
        def _():
            remote(src, src, number(key), shift).wait_send()

    def along(axis, side):
        shift = [0, 0, 0]
        shift[axis] = 1 if side == 0 else -1
        return shift

    def x_plane(near, side):
        return nx - near if side == 0 else 1 + near

    def send_x(k, wanted=None):
        for side in range(2):
            start(("x", k, side), search.at[k, :, x_plane(1, side), own],
                  xin.at[k, side], along(0, side), wanted)

    def send_y(k, wanted=None):
        for side in range(2):
            start(("y", k, side), yout.at[k, side], yin.at[k, side], along(1, side), wanted)

    def send_c(k, wanted=None):
        for cx in range(2):
            for cy in range(2):
                shift = [1 - 2 * cx, 1 - 2 * cy, 0]
                start(("c", k, cx, cy), cout.at[k, cx, cy], cin.at[k, cx, cy], shift, wanted)

    def send_z(k, kind, packs, wanted=None):
        for side in range(2):
            zout[k, kind, side] = packs[side]
            start(("z", k, kind, side), zout.at[k, kind, side], zin.at[k, kind, side],
                  along(2, side), wanted)

    def take_x(k):
        for side in range(2):
            arrive(("x", k, side), xin.at[k, side], along(0, side))

    def take_y(k):
        for side in range(2):
            arrive(("y", k, side), yin.at[k, side], along(1, side))

    def take_c(k):
        for cx in range(2):
            for cy in range(2):
                arrive(("c", k, cx, cy), cin.at[k, cx, cy], [1 - 2 * cx, 1 - 2 * cy, 0])

    def take_z(k, kind):
        for side in range(2):
            arrive(("z", k, kind, side), zin.at[k, kind, side], along(2, side))

    def precondition(scale, mass, vector):
        value, density = [None] * levels, [None] * levels
        carry = None
        for t in range(levels - 1, -1, -1):
            carry = vector[t] if carry is None else vector[t] + carry
            carry = carry * scale(t)
            value[t] = carry
        carry = None
        for t in range(levels):
            push = vector[levels + t] + (6.0 * mass(t)) * value[t]
            carry = push if carry is None else push + carry
            carry = carry * scale(t)
            density[t] = carry
        return value + density

    def mix(founds):
        blends = []
        for odd in range(2):
            whole = jnp.concatenate([found[f] for found in founds for f in range(odd, fields, 2)], 0)
            high = whole.astype(jnp.bfloat16)
            low = (whole - high.astype(jnp.float32)).astype(jnp.bfloat16)
            blends.append(jnp.dot(
                jnp.concatenate([high, low], 1), mixer[odd], preferred_element_type=jnp.float32
            ))
        mixed = []
        for place in range(len(founds)):
            parts = []
            for f in range(fields):
                row = (place * (fields // 2) + f // 2) * ny
                parts.append((blends[f % 2][row : row + ny, :nz], blends[f % 2][row : row + ny, nz:]))
            mixed.append(parts)
        return mixed

    def pack(packs, base, mixed):
        high, low = packs
        for f in range(fields):
            place = base + f
            high = jnp.where(lane == place, mixed[f][1], high)
            low = jnp.where(next_lane == place, mixed[f][1], low)
        return high, low

    def advance(k, kind, base, center, low, high, below, above, beyond, mass, pull, prior):
        zlow, zhigh = zin.at[k, kind, 0], zin.at[k, kind, 1]

        def around(f):
            place = base + f
            edge = jnp.where(lane == place, zlow[...], zhigh[...])
            edge = jnp.where(ends_mask, pltpu.roll(edge, (nz - place) & (nz - 1), 1), 0.0)
            return ((below(f) + above(f)) + (low(f) + high(f))) + (beyond(f) + edge)

        found = [None] * fields
        for t in range(levels):
            value = around(t)
            density = around(levels + t) - mass(t) * value
            value = value + pull(t) * center(levels + t)
            for f, item in ((t, value), (levels + t, density)):
                found[f] = SCALE * item - BACK * prior(f)
        return found

    def publish(k, x, found, fixed):
        for f in range(fields):
            search[k, f, x + 1, own] = found[f]
            for side, (edge, near) in enumerate(((0, ny - 2), (ny - 1, 1))):
                rows[k, side, f, pl.ds(x, 1), :] = found[f][edge : edge + 1, :]
                yout[k, side, f, pl.ds(x, 1), :] = found[f][near : near + 1, :]
            if fixed is not None:
                for cy in range(2):
                    edge = ny - 1 if cy == 0 else 0
                    cout[k, fixed, cy, f : f + 1, :] = found[f][edge : edge + 1, :]

    def own_planes(k, planes, packs):
        before = k * lax.div(lax.div(k, 2) + ITERS - 2, ITERS - 1)
        founds = []
        for x, fixed in planes:
            vector = advance(
                k, 0, x * fields,
                lambda f: search[k, f, x + 1, own],
                lambda f: search[k, f, x + 1, pl.ds(PAD - 1, ny)],
                lambda f: search[k, f, x + 1, pl.ds(PAD + 1, ny)],
                lambda f: search[k, f, x, own],
                lambda f: search[k, f, x + 2, own],
                lambda f: zsum[lax.rem(k, 2), f, x + 1],
                lambda t: weight[t, x],
                lambda t: couple[t, x],
                lambda f: basis[before, f, x, plane],
            )
            for f in range(fields):
                basis[k + 2, f, x, plane] = vector[f]
            founds.append(
                precondition(lambda t: inv[t, x], lambda t: weight[t, x], vector)
            )
        return spread(k + 1, planes, founds, packs)

    def spread(k, planes, founds, packs):
        for (x, fixed), found, mixed in zip(planes, founds, mix(founds)):
            packs = pack(packs, x * fields, mixed)
            publish(k, x, found, fixed)
            for f in range(fields):
                zsum[lax.rem(k, 2), f, x + 1] = mixed[f][0]
        return packs

    def scatter(k, side, get):
        row = PAD - 1 if side == 0 else PAD + ny
        for f in range(fields):
            found = get(f)
            for x in range(nx):
                search[k, f, x + 1, row : row + 1, :] = found[x : x + 1, :]

    def aside(k, side, found, packs):
        mixed = mix([found])[0]
        for f in range(fields):
            zside[lax.rem(k, 2), side, f] = mixed[f][0]
        return pack(packs, side * fields, mixed)

    def across(k, side, edge, found, packs):
        mixed = mix([found])[0]
        for f in range(fields):
            zsum[lax.rem(k, 2), f, edge] = mixed[f][0]
        return pack(packs, side * fields, mixed)

    def y_given():
        packs = (blank, blank)
        for side in range(2):
            arrive(("y0", side), beside.at[0, side, :, own], along(1, side))
        for side in range(2):
            found = [beside[0, side, f, own] for f in range(fields)]
            scatter(0, side, lambda f: found[f])
            packs = aside(0, side, found, packs)
        send_z(0, 1, packs)
        for axis, ghost in enumerate((ghost_x, ghost_y)):
            for side in range(2):
                arrive(("gx" if axis == 0 else "gy", side), ghost.at[side], along(axis, side))
                there = index[axis] > 0 if side == 0 else index[axis] < sizes[axis] - 1
                for t in range(levels):
                    ghost_inv[axis, side, t] = jnp.where(
                        there, 1.0 / (time_rate + 6.0 + ghost[side, 0, t]), 0.0
                    )

    def y_ghosts(k):
        packs = (blank, blank)
        j = k - 1
        take_y(j)
        take_c(j)
        take_z(j, 1)
        for side in range(2):
            for f in range(fields):
                beside[j, side, f, PAD - 1 : PAD, :] = cin[j, 0, side, f : f + 1, :]
                beside[j, side, f, PAD + nx : PAD + nx + 1, :] = cin[j, 1, side, f : f + 1, :]
            vector = advance(
                j, 1, side * fields,
                lambda f: beside[j, side, f, own],
                lambda f: beside[j, side, f, pl.ds(PAD - 1, nx)],
                lambda f: beside[j, side, f, pl.ds(PAD + 1, nx)],
                lambda f: yin[j, side, f],
                lambda f: rows[j, side, f],
                lambda f: zside[lax.rem(j, 2), side, f],
                lambda t: ghost_y[side, 1, t],
                lambda t: ghost_y[side, 2, t],
                lambda f: past[lax.rem(k, 2), 1, side, f],
            )
            for f in range(fields):
                past[lax.rem(k, 2), 1, side, f] = vector[f]
            found = precondition(
                lambda t: ghost_inv[1, side, t], lambda t: ghost_y[side, 1, t], vector
            )
            for f in range(fields):
                beside[k, side, f, own] = found[f]
            scatter(k, side, lambda f: found[f])
            packs = aside(k, side, found, packs)
        send_z(k, 1, packs, k < ITERS - 1)

    def x_given():
        packs = (blank, blank)
        for side in range(2):
            edge = nx + 1 if side else 0
            arrive(("x0", side), search.at[0, :, edge, own], along(0, side))
            found = [search[0, f, edge, own] for f in range(fields)]
            packs = across(0, side, edge, found, packs)
        send_z(0, 2, packs)

    def x_ghosts(k):
        packs = (blank, blank)
        j = k - 1
        take_x(j)
        take_z(j, 2)
        for side in range(2):
            edge, inner = (0, 1) if side == 0 else (nx + 1, nx)
            for f in range(fields):
                search[j, f, edge, PAD - 1 : PAD, :] = cin[j, side, 0, f : f + 1, :]
                search[j, f, edge, PAD + ny : PAD + ny + 1, :] = cin[j, side, 1, f : f + 1, :]
            vector = advance(
                j, 2, side * fields,
                lambda f: search[j, f, edge, own],
                lambda f: search[j, f, edge, pl.ds(PAD - 1, ny)],
                lambda f: search[j, f, edge, pl.ds(PAD + 1, ny)],
                lambda f: xin[j, side, f],
                lambda f: search[j, f, inner, own],
                lambda f: zsum[lax.rem(j, 2), f, edge],
                lambda t: ghost_x[side, 1, t],
                lambda t: ghost_x[side, 2, t],
                lambda f: past[lax.rem(k, 2), 0, side, f],
            )
            for f in range(fields):
                past[lax.rem(k, 2), 0, side, f] = vector[f]
            found = precondition(
                lambda t: ghost_inv[0, side, t], lambda t: ghost_x[side, 1, t], vector
            )
            for f in range(fields):
                search[k, f, edge, own] = found[f]
            packs = across(k, side, edge, found, packs)
        send_z(k, 2, packs, k < ITERS - 1)

    def dots(k):
        def group(g, carry):
            def step(place, accs):
                sums = [[] for _ in range(GROUP)]
                for x in range(SPAN):
                    x = place * SPAN + x
                    mine = [basis[k + 1, f, x, plane] for f in range(fields)]
                    for i in range(GROUP):
                        terms = [mine[f] * basis[g * GROUP + i + 1, f, x, plane] for f in range(fields)]
                        while len(terms) > 1:
                            terms = [a + b for a, b in zip(terms[::2], terms[1::2])]
                        sums[i].append(terms[0])
                return tuple(acc + sum(more) for acc, more in zip(accs, sums))

            accs = lax.fori_loop(0, nx // SPAN, step, (blank,) * GROUP)
            for i in range(GROUP):
                row = gram_row(g * GROUP + i, k)
                gram[pl.ds(row, 1), :] = jnp.sum(accs[i], axis=0, keepdims=True)
            return carry

        lax.fori_loop(0, lax.div(k, GROUP) + 1, group, 0)

    for load in loads:
        load.wait()

    def invert(x, carry):
        for t in range(levels):
            inv[t, x] = 1.0 / (time_rate + 6.0 + coef[0, t, x])
            for which in range(3):
                item = coef[which, t, x]
                given[0, which, t, pl.ds(x, 1), :] = item[ny - 1 : ny, :]
                given[1, which, t, pl.ds(x, 1), :] = item[0:1, :]
        return carry

    lax.fori_loop(0, nx, invert, 0)
    def first(planes, packs):
        founds = [
            precondition(
                lambda t: inv[t, x], lambda t: weight[t, x],
                [basis[1, f, x, plane] for f in range(fields)],
            )
            for x, _ in planes
        ]
        return spread(0, planes, founds, packs)

    def sweep(body, packs, low):
        return lax.fori_loop(
            0, (nx - 2 * low) // PLANES,
            lambda step, packs: body(
                [(low + step * PLANES + place, None) for place in range(PLANES)], packs
            ),
            packs,
        )

    pl.semaphore_wait(barrier, total - 1)
    for side in range(2):
        start(("gx", side), coef.at[:, :, nx - 1 if side == 0 else 0], ghost_x.at[side],
              along(0, side))
    for side in range(2):
        start(("gy", side), given.at[side], ghost_y.at[side], along(1, side))
    from_lane = lax.broadcasted_iota(jnp.int32, (2 * nz, 2 * nz), 0) & (nz - 1)
    to_lane = lax.broadcasted_iota(jnp.int32, (2 * nz, 2 * nz), 1)
    for odd in range(2):
        beside_lane = jnp.logical_or(from_lane - to_lane == 1, to_lane - from_lane == 1)
        last_lane = jnp.logical_and((to_lane & 1) == odd, from_lane == nz - 1)
        first_lane = jnp.logical_and((to_lane & 1) != odd, from_lane == 0)
        taken = jnp.where(
            to_lane < nz, beside_lane.astype(jnp.int32),
            jnp.logical_or(last_lane, first_lane).astype(jnp.int32),
        )
        mixer[odd] = taken.astype(jnp.float32).astype(jnp.bfloat16)
    ends = [(0, 1), (nx - 1, 0)]
    packs = first(ends, (blank, blank))
    packs = first([(1, None), (nx - 2, None)], packs)
    packs = sweep(first, packs, 2)
    for side in range(2):
        start(("x0", side), search.at[0, :, nx if side == 0 else 1, own],
              search.at[0, :, nx + 1 if side else 0, own], along(0, side))
    for side in range(2):
        start(("y0", side), rows.at[0, 1 - side], beside.at[0, side, :, own], along(1, side))
    send_z(0, 0, packs)
    send_c(0)
    send_x(0)
    send_y(0)
    dots(0)
    y_given()

    def iterate(k, carry):
        more = k < ITERS - 2

        @pl.when(k > 0)
        def _():
            y_ghosts(k)

        take_z(k, 0)
        body = functools.partial(own_planes, k)
        packs = body([(1, None), (nx - 2, None)], (blank, blank))
        send_x(k + 1, more)
        packs = sweep(body, packs, 2)

        @pl.when(k == 0)
        def _():
            x_given()

        @pl.when(k > 0)
        def _():
            x_ghosts(k)

        packs = body(ends, packs)
        send_z(k + 1, 0, packs, k < ITERS - 1)
        send_c(k + 1, more)
        send_y(k + 1, more)
        dots(k + 1)
        return carry

    lax.fori_loop(0, ITERS, iterate, 0)

    def settle(k, carry):
        more = k < ITERS - 1
        for side in range(2):
            drain(("x", k, side), xin.at[k, side], along(0, side), more)
            drain(("y", k, side), yin.at[k, side], along(1, side), more)
            for cy in range(2):
                drain(("c", k, side, cy), cin.at[k, side, cy], [1 - 2 * side, 1 - 2 * cy, 0], more)
            for kind in range(3):
                drain(("z", k, kind, side), zin.at[k, kind, side], along(2, side),
                      None if kind == 0 else more)
        return carry

    lax.fori_loop(0, ITERS, settle, 0)
    for side in range(2):
        drain(("x0", side), search.at[0, :, 0, own], along(0, side))
        drain(("y0", side), beside.at[0, side, :, own], along(1, side))
        drain(("gx", side), ghost_x.at[side], along(0, side))
        drain(("gy", side), ghost_y.at[side], along(1, side))

    local = jnp.sum(gram[...].T, axis=0, keepdims=True)
    gsend[...] = local
    gall[me] = local

    def spread(step, carry):
        pltpu.make_async_remote_copy(
            src_ref=gsend, dst_ref=gall.at[me], send_sem=gssem, recv_sem=grsem,
            device_id=ident((me + step) % total), device_id_type=pl.DeviceIdType.MESH,
        ).start()
        return carry

    lax.fori_loop(1, total, spread, 0)
    others = gall.at[pl.ds(0, total - 1)]
    pltpu.make_async_copy(others, others, grsem).wait()
    pltpu.make_async_copy(others, others, gssem).wait()
    whole = jnp.sum(gall[...], axis=0)
    splat[...] = jnp.broadcast_to(whole, splat.shape).T

    def entry(i, j):
        row = gram_row(i, j)
        return splat[row : row + 1, :]

    solved, worst = gram_solve(entry, ITERS)
    flag[...] = jnp.broadcast_to(worst, flag.shape)

    def combine(x, carry):
        for f in range(fields):
            item = solved[0] * search[0, f, x + 1, own]
            for k in range(1, ITERS):
                item = item + solved[k] * search[k, f, x + 1, own]
            ready[f, x] = item
        pltpu.make_async_copy(ready.at[:, x], out.at[:, x], osem).start()
        return carry

    lax.fori_loop(0, nx, combine, 0)
    pltpu.make_async_copy(ready, out, osem).wait()


def fused(sizes, residual, reaction, transport, congestion):
    levels, nx, ny, nz = reaction.shape
    fields = 2 * levels
    total = sizes[0] * sizes[1] * sizes[2]
    pairs = (ITERS + 1) ** 2
    assert (ITERS + 1) % GROUP == 0
    assert fields * nx <= nz and pairs <= nz and (nx - 4) % PLANES == 0 and nx == ny
    assert nz & (nz - 1) == 0
    f32 = jnp.float32
    hbm = pl.BlockSpec(memory_space=pl.ANY)
    vmem = pl.BlockSpec(memory_space=pltpu.VMEM)
    wide = ny + 3 * PAD
    copies = sum(width * cycle for _, width, cycle in CHANNELS.values()) + 2 * len(STARTS)
    out, flag = pl.pallas_call(
        functools.partial(kernel, levels, sizes),
        out_shape=(
            jax.ShapeDtypeStruct((fields, nx, ny, nz), f32),
            jax.ShapeDtypeStruct((8, nz), f32),
        ),
        in_specs=[hbm] * 4,
        out_specs=(hbm, vmem),
        scratch_shapes=[
            pltpu.VMEM((ITERS + 2, fields, nx + 1, ny + PAD, nz), f32),
            pltpu.VMEM((3, levels, nx, ny, nz), f32),
            pltpu.VMEM((levels, nx, ny, nz), f32),
            pltpu.VMEM((ITERS + 1, fields, nx + 2, wide, nz), f32),
            pltpu.VMEM((ITERS, 2, fields, wide, nz), f32),
            pltpu.VMEM((ITERS + 1, 2, fields, ny, nz), f32),
            pltpu.VMEM((ITERS + 1, 2, fields, nx, nz), f32),
            pltpu.VMEM((ITERS + 1, 2, fields, nx, nz), f32),
            pltpu.VMEM((ITERS + 1, 2, fields, nx, nz), f32),
            pltpu.VMEM((ITERS + 1, 2, 2, fields, nz), f32),
            pltpu.VMEM((ITERS + 1, 2, 2, fields, nz), f32),
            pltpu.VMEM((ITERS + 1, 3, 2, ny, nz), f32),
            pltpu.VMEM((ITERS + 1, 3, 2, ny, nz), f32),
            pltpu.VMEM((2, 3, levels, ny, nz), f32),
            pltpu.VMEM((2, 3, levels, nx, nz), f32),
            pltpu.VMEM((2, 2, levels, ny, nz), f32),
            pltpu.VMEM((2, 3, levels, nx, nz), f32),
            pltpu.VMEM((2, 2, 2, fields, ny, nz), f32),
            pltpu.VMEM((2, 2 * nz, 2 * nz), jnp.bfloat16),
            pltpu.VMEM((2, fields, nx + 2, ny, nz), f32),
            pltpu.VMEM((2, 2, fields, nx, nz), f32),
            pltpu.VMEM((nz, nz), f32),
            pltpu.VMEM((nz, nz), f32),
            pltpu.VMEM((1, nz), f32),
            pltpu.VMEM((total, 1, nz), f32),
            pltpu.VMEM((fields, nx, ny, nz), f32),
            pltpu.SemaphoreType.DMA((4,)),
            pltpu.SemaphoreType.DMA,
            pltpu.SemaphoreType.DMA((copies,)),
            pltpu.SemaphoreType.DMA,
            pltpu.SemaphoreType.DMA,
            pltpu.SemaphoreType.DMA,
        ],
        compiler_params=pltpu.CompilerParams(
            collective_id=0, has_side_effects=True, vmem_limit_bytes=60 * 1024 * 1024
        ),
        name="krylov",
    )(residual.reshape((fields, nx, ny, nz)), reaction, transport, congestion)
    return out.reshape(residual.shape), flag


def neighbours(field):
    total = 0.0
    for axis, dim in (("gx", 2), ("gy", 3), ("gz", 4)):
        count = lax.axis_size(axis)
        size = field.shape[dim]
        forward = [(i, i + 1) for i in range(count - 1)]
        backward = [(target, source) for source, target in forward]
        low = lax.ppermute(lax.slice_in_dim(field, size - 1, size, axis=dim), axis, forward)
        high = lax.ppermute(lax.slice_in_dim(field, 0, 1, axis=dim), axis, backward)
        below = jnp.concatenate([low, lax.slice_in_dim(field, 0, size - 1, axis=dim)], dim)
        above = jnp.concatenate([lax.slice_in_dim(field, 1, size, axis=dim), high], dim)
        total = total + below + above
    return total


def jacobian(vector, reaction, transport, congestion):
    lapped = 6.0 * vector - neighbours(vector)
    value_part, density_part = (vector[0], vector[1])
    later = jnp.concatenate([value_part[1:], jnp.zeros_like(value_part[:1])], 0)
    earlier = jnp.concatenate([jnp.zeros_like(density_part[:1]), density_part[:-1]], 0)
    first = (
        time_rate * (value_part - later)
        + lapped[0]
        + reaction * value_part
        - congestion * density_part
    )
    second = (
        time_rate * (density_part - earlier)
        + lapped[1]
        + reaction * density_part
        - transport * lapped[0]
    )
    return jnp.stack([first, second], 0)


def precondition(vector, reaction, transport):
    levels = vector.shape[1]
    diag = time_rate + 6.0 + reaction
    value_levels = [None] * levels
    carry = jnp.zeros_like(vector[0, 0])
    for level in range(levels - 1, -1, -1):
        carry = (vector[0, level] + time_rate * carry) / diag[level]
        value_levels[level] = carry
    density_levels = []
    carry = jnp.zeros_like(vector[1, 0])
    for level in range(levels):
        carry = (
            vector[1, level] + time_rate * carry + 6.0 * transport[level] * value_levels[level]
        ) / diag[level]
        density_levels.append(carry)
    return jnp.stack([jnp.stack(value_levels, 0), jnp.stack(density_levels, 0)], 0)


def arnoldi(residual, reaction, transport, congestion):
    dims = tuple(range(1, residual.ndim + 1))
    beta = jnp.sqrt(lax.psum(jnp.sum(residual * residual), AXES))
    basis = jnp.zeros((ITERS + 1,) + residual.shape, residual.dtype).at[0].set(residual / beta)
    heights = jnp.zeros((ITERS, ITERS + 1), residual.dtype)

    def step(c, state):
        basis, heights = state
        search = precondition(basis[c], reaction, transport)
        image = jacobian(search, reaction, transport, congestion)
        coeffs = lax.psum(jnp.sum(basis * image[None], axis=dims), AXES)
        image = image - jnp.sum(coeffs.reshape((-1,) + (1,) * residual.ndim) * basis, axis=0)
        height = jnp.sqrt(lax.psum(jnp.sum(image * image), AXES))
        basis = basis.at[c + 1].set(image / height)
        return basis, heights.at[c].set(coeffs.at[c + 1].set(height))

    basis, heights = lax.fori_loop(0, ITERS, step, (basis, heights))
    columns = [[heights[c, i] for i in range(c + 2)] for c in range(ITERS)]
    solved = least_squares(columns, beta, ITERS)
    mixed = sum(solved[c] * basis[c] for c in range(ITERS))
    return precondition(mixed, reaction, transport)


def body(sizes, residual_in, reaction, transport, congestion):
    update, flag = fused(sizes, residual_in, reaction, transport, congestion)
    return lax.cond(
        flag[0, 0] > PIVOT,
        lambda update, *rest: update,
        lambda update, *rest: arnoldi(*rest),
        update, residual_in, reaction, transport, congestion,
    )


def solution(mesh):
    placed = (
        P(None, None, "gx", "gy", "gz"),
        P(None, "gx", "gy", "gz"),
        P(None, "gx", "gy", "gz"),
        P(None, "gx", "gy", "gz"),
    )
    sizes = tuple(mesh.shape[axis] for axis in AXES)
    return jax.shard_map(
        functools.partial(body, sizes), mesh=mesh, in_specs=placed,
        out_specs=P(None, None, "gx", "gy", "gz"), check_vma=False,
    )
```

```python
import functools

import jax
import jax.numpy as jnp
from jax import lax
from jax.experimental import pallas as pl
from jax.experimental.pallas import tpu as pltpu
from jax.sharding import PartitionSpec as P

ITERS = 8
AXES = ("gx", "gy", "gz")
time_rate = 1.0
SCALE = 2.5
BACK = 1.0
PIVOT = 2.5e-3
PLANES = 6
PAD = 8
FIRST_BACK = 2
GROUP = 3
SPAN = 4
STARTS = ("x0", "y0", "gx", "gy")
CHANNELS = {
    "x": (8, 2, ITERS),
    "y": (24, 2, 4),
    "c": (32, 4, 4),
    ("z", 0): (48, 2, 2),
    ("z", 1): (52, 2, 4),
    ("z", 2): (60, 2, 2),
}


def gram_row(row, column):
    return column * (ITERS + 1) + row


def least_squares(columns, beta, steps):
    zero = jnp.zeros_like(beta)
    rotations = []
    target = [beta] + [zero] * steps
    upper = []
    for column_index in range(steps):
        column = list(columns[column_index])
        for place, (cosine, sine) in enumerate(rotations):
            upper_entry = cosine * column[place] + sine * column[place + 1]
            lower_entry = -sine * column[place] + cosine * column[place + 1]
            column[place], column[place + 1] = (upper_entry, lower_entry)
        radius = jnp.sqrt(column[column_index] ** 2 + column[column_index + 1] ** 2)
        inverse = 1.0 / radius
        cosine = column[column_index] * inverse
        sine = column[column_index + 1] * inverse
        column[column_index] = inverse
        rotations.append((cosine, sine))
        target[column_index], target[column_index + 1] = (
            cosine * target[column_index],
            -sine * target[column_index],
        )
        upper.append(column[: column_index + 1])
    solved = [None] * steps
    for row_index in range(steps - 1, -1, -1):
        accum = target[row_index]
        for later_index in range(steps - 1, row_index, -1):
            accum = accum - upper[later_index][row_index] * solved[later_index]
        solved[row_index] = accum * upper[row_index][row_index]
    return solved


def gram_solve(gram, steps):
    size = steps + 1
    work = {(i, j): gram(i, j) for j in range(size) for i in range(j + 1)}
    factor = {}
    worst = None
    for i in range(size):
        ratio = work[i, i] / gram(i, i)
        worst = ratio if worst is None else jnp.where(ratio > worst, worst, ratio)
        pivot = jnp.sqrt(work[i, i])
        inverse = 1.0 / pivot
        factor[i, i] = pivot
        for j in range(i + 1, size):
            factor[i, j] = work[i, j] * inverse
        for a in range(i + 1, size):
            for b in range(a, size):
                work[a, b] = work[a, b] - factor[i, a] * factor[i, b]
    columns = []
    for k in range(steps):
        column = []
        for i in range(k + 2):
            entry = -factor[i, k + 1] * (1.0 / SCALE)
            if i <= k:
                entry = entry + factor[i, k]
            if k >= FIRST_BACK and i <= k - 1:
                entry = entry - factor[i, k - 1] * (BACK / SCALE)
            column.append(entry)
        columns.append(column)
    return least_squares(columns, factor[0, 0], steps), worst


def kernel(
    levels, sizes, residual, reaction, transport, congestion, out, flag,
    basis, coef, inv, search, beside, xin, yin, yout, rows, cin, cout, zin, zout,
    ghost_x, ghost_y, ghost_inv, given, past, mixer, zsum, zside, gram, splat, gsend, gall,
    ready, insem, ssem, rsem, gssem, grsem, osem,
):
    fields = 2 * levels
    nx, ny, nz = residual.shape[1:]
    total = sizes[0] * sizes[1] * sizes[2]
    index = [lax.axis_index(axis) for axis in AXES]
    me = (index[0] * sizes[1] + index[1]) * sizes[2] + index[2]
    lane = lax.broadcasted_iota(jnp.int32, (ny, nz), 1)
    plane = pl.ds(0, ny)
    next_lane = (lane + 1) & (nz - 1)
    ends_mask = jnp.logical_or(lane == 0, lane == nz - 1)
    own = pl.ds(PAD, ny)
    blank = jnp.zeros((ny, nz), jnp.float32)
    weight, couple = coef.at[1], coef.at[2]

    loads = [
        pltpu.make_async_copy(src, dst, insem.at[place])
        for place, (src, dst) in enumerate((
            (residual, basis.at[1, :, pl.ds(0, nx), pl.ds(0, ny)]), (reaction, coef.at[0]),
            (transport, coef.at[1]), (congestion, coef.at[2]),
        ))
    ]
    for load in loads:
        load.start()

    for buffer in (xin, yin, cin, zin, ghost_x, ghost_y):
        buffer[...] = jnp.zeros_like(buffer)
    for slot in range(2):
        edge = nx + 1 if slot else 0
        search[0, :, edge] = jnp.zeros_like(search[0, :, edge])
    beside[0] = jnp.zeros_like(beside[0])
    past[...] = jnp.zeros_like(past)
    basis[0] = jnp.zeros_like(basis[0])
    gram[...] = jnp.zeros_like(gram)

    def ident(other):
        return (other // (sizes[1] * sizes[2]), (other // sizes[2]) % sizes[1], other % sizes[2])

    barrier = pltpu.get_barrier_semaphore()

    def greet(step, carry):
        pl.semaphore_signal(
            barrier, inc=1, device_id=ident((me + step) % total),
            device_id_type=pl.DeviceIdType.MESH,
        )
        return carry

    lax.fori_loop(1, total, greet, 0)

    def reaches(shift):
        ok = None
        for axis, move in enumerate(shift):
            if move == 0:
                continue
            this = index[axis] < sizes[axis] - 1 if move > 0 else index[axis] > 0
            ok = this if ok is None else jnp.logical_and(ok, this)
        return ok

    def remote(src, dst, place, shift):
        return pltpu.make_async_remote_copy(
            src_ref=src, dst_ref=dst, send_sem=ssem, recv_sem=rsem.at[place],
            device_id=tuple(i + move for i, move in zip(index, shift)),
            device_id_type=pl.DeviceIdType.MESH,
        )

    def number(key):
        kind, rest = key[0], key[1:]
        if kind in STARTS:
            return 2 * STARTS.index(kind) + rest[0]
        base, width, cycle = CHANNELS[kind if kind != "z" else (kind, rest[1])]
        spot = 0
        for part in rest[2 if kind == "z" else 1 :]:
            spot = 2 * spot + part
        return base + lax.rem(rest[0], cycle) * width + spot

    def start(key, src, dst, shift, wanted=None):
        go = reaches(shift)

        @pl.when(go if wanted is None else jnp.logical_and(go, wanted))
        def _():
            remote(src, dst, number(key), shift).start()

    def arrive(key, dst, shift):
        @pl.when(reaches([-move for move in shift]))
        def _():
            remote(dst, dst, number(key), shift).wait_recv()

    def drain(key, src, shift, wanted=None):
        go = reaches(shift)

        @pl.when(go if wanted is None else jnp.logical_and(go, wanted))
        def _():
            remote(src, src, number(key), shift).wait_send()

    def along(axis, side):
        shift = [0, 0, 0]
        shift[axis] = 1 if side == 0 else -1
        return shift

    def x_plane(near, side):
        return nx - near if side == 0 else 1 + near

    def send_x(k, wanted=None):
        for side in range(2):
            start(("x", k, side), search.at[k, :, x_plane(1, side), own],
                  xin.at[k, side], along(0, side), wanted)

    def send_y(k, wanted=None):
        for side in range(2):
            start(("y", k, side), yout.at[k, side], yin.at[k, side], along(1, side), wanted)

    def send_c(k, wanted=None):
        for cx in range(2):
            for cy in range(2):
                shift = [1 - 2 * cx, 1 - 2 * cy, 0]
                start(("c", k, cx, cy), cout.at[k, cx, cy], cin.at[k, cx, cy], shift, wanted)

    def send_z(k, kind, packs, wanted=None):
        for side in range(2):
            zout[k, kind, side] = packs[side]
            start(("z", k, kind, side), zout.at[k, kind, side], zin.at[k, kind, side],
                  along(2, side), wanted)

    def take_x(k):
        for side in range(2):
            arrive(("x", k, side), xin.at[k, side], along(0, side))

    def take_y(k):
        for side in range(2):
            arrive(("y", k, side), yin.at[k, side], along(1, side))

    def take_c(k):
        for cx in range(2):
            for cy in range(2):
                arrive(("c", k, cx, cy), cin.at[k, cx, cy], [1 - 2 * cx, 1 - 2 * cy, 0])

    def take_z(k, kind):
        for side in range(2):
            arrive(("z", k, kind, side), zin.at[k, kind, side], along(2, side))

    def precondition(scale, mass, vector):
        value, density = [None] * levels, [None] * levels
        carry = None
        for t in range(levels - 1, -1, -1):
            carry = vector[t] if carry is None else vector[t] + carry
            carry = carry * scale(t)
            value[t] = carry
        carry = None
        for t in range(levels):
            push = vector[levels + t] + (6.0 * mass(t)) * value[t]
            carry = push if carry is None else push + carry
            carry = carry * scale(t)
            density[t] = carry
        return value + density

    def mix(founds):
        blends = []
        for odd in range(2):
            whole = jnp.concatenate([found[f] for found in founds for f in range(odd, fields, 2)], 0)
            high = whole.astype(jnp.bfloat16)
            low = (whole - high.astype(jnp.float32)).astype(jnp.bfloat16)
            blends.append(jnp.dot(
                jnp.concatenate([high, low], 1), mixer[odd], preferred_element_type=jnp.float32
            ))
        mixed = []
        for place in range(len(founds)):
            parts = []
            for f in range(fields):
                row = (place * (fields // 2) + f // 2) * ny
                parts.append((blends[f % 2][row : row + ny, :nz], blends[f % 2][row : row + ny, nz:]))
            mixed.append(parts)
        return mixed

    def pack(packs, base, mixed):
        high, low = packs
        for f in range(fields):
            place = base + f
            high = jnp.where(lane == place, mixed[f][1], high)
            low = jnp.where(next_lane == place, mixed[f][1], low)
        return high, low

    def advance(k, kind, base, center, low, high, below, above, beyond, mass, pull, prior):
        zlow, zhigh = zin.at[k, kind, 0], zin.at[k, kind, 1]

        def around(f):
            place = base + f
            edge = jnp.where(lane == place, zlow[...], zhigh[...])
            edge = jnp.where(ends_mask, pltpu.roll(edge, (nz - place) & (nz - 1), 1), 0.0)
            return ((below(f) + above(f)) + (low(f) + high(f))) + (beyond(f) + edge)

        found = [None] * fields
        for t in range(levels):
            value = around(t)
            density = around(levels + t) - mass(t) * value
            value = value + pull(t) * center(levels + t)
            for f, item in ((t, value), (levels + t, density)):
                found[f] = SCALE * item - BACK * prior(f)
        return found

    def publish(k, x, found, fixed):
        for f in range(fields):
            search[k, f, x + 1, own] = found[f]
            for side, (edge, near) in enumerate(((0, ny - 2), (ny - 1, 1))):
                rows[k, side, f, pl.ds(x, 1), :] = found[f][edge : edge + 1, :]
                yout[k, side, f, pl.ds(x, 1), :] = found[f][near : near + 1, :]
            if fixed is not None:
                for cy in range(2):
                    edge = ny - 1 if cy == 0 else 0
                    cout[k, fixed, cy, f : f + 1, :] = found[f][edge : edge + 1, :]

    def own_planes(k, planes, packs):
        before = k * lax.div(lax.div(k, 2) + ITERS - 2, ITERS - 1)
        founds = []
        for x, fixed in planes:
            vector = advance(
                k, 0, x * fields,
                lambda f: search[k, f, x + 1, own],
                lambda f: search[k, f, x + 1, pl.ds(PAD - 1, ny)],
                lambda f: search[k, f, x + 1, pl.ds(PAD + 1, ny)],
                lambda f: search[k, f, x, own],
                lambda f: search[k, f, x + 2, own],
                lambda f: zsum[lax.rem(k, 2), f, x + 1],
                lambda t: weight[t, x],
                lambda t: couple[t, x],
                lambda f: basis[before, f, x, plane],
            )
            for f in range(fields):
                basis[k + 2, f, x, plane] = vector[f]
            founds.append(
                precondition(lambda t: inv[t, x], lambda t: weight[t, x], vector)
            )
        return spread(k + 1, planes, founds, packs)

    def spread(k, planes, founds, packs):
        for (x, fixed), found, mixed in zip(planes, founds, mix(founds)):
            packs = pack(packs, x * fields, mixed)
            publish(k, x, found, fixed)
            for f in range(fields):
                zsum[lax.rem(k, 2), f, x + 1] = mixed[f][0]
        return packs

    def scatter(k, side, get):
        row = PAD - 1 if side == 0 else PAD + ny
        for f in range(fields):
            found = get(f)
            for x in range(nx):
                search[k, f, x + 1, row : row + 1, :] = found[x : x + 1, :]

    def aside(k, side, found, packs):
        mixed = mix([found])[0]
        for f in range(fields):
            zside[lax.rem(k, 2), side, f] = mixed[f][0]
        return pack(packs, side * fields, mixed)

    def across(k, side, edge, found, packs):
        mixed = mix([found])[0]
        for f in range(fields):
            zsum[lax.rem(k, 2), f, edge] = mixed[f][0]
        return pack(packs, side * fields, mixed)

    def y_given():
        packs = (blank, blank)
        for side in range(2):
            arrive(("y0", side), beside.at[0, side, :, own], along(1, side))
        for side in range(2):
            found = [beside[0, side, f, own] for f in range(fields)]
            scatter(0, side, lambda f: found[f])
            packs = aside(0, side, found, packs)
        send_z(0, 1, packs)
        for axis, ghost in enumerate((ghost_x, ghost_y)):
            for side in range(2):
                arrive(("gx" if axis == 0 else "gy", side), ghost.at[side], along(axis, side))
                there = index[axis] > 0 if side == 0 else index[axis] < sizes[axis] - 1
                for t in range(levels):
                    ghost_inv[axis, side, t] = jnp.where(
                        there, 1.0 / (time_rate + 6.0 + ghost[side, 0, t]), 0.0
                    )

    def y_ghosts(k):
        packs = (blank, blank)
        j = k - 1
        take_y(j)
        take_c(j)
        take_z(j, 1)
        for side in range(2):
            for f in range(fields):
                beside[j, side, f, PAD - 1 : PAD, :] = cin[j, 0, side, f : f + 1, :]
                beside[j, side, f, PAD + nx : PAD + nx + 1, :] = cin[j, 1, side, f : f + 1, :]
            vector = advance(
                j, 1, side * fields,
                lambda f: beside[j, side, f, own],
                lambda f: beside[j, side, f, pl.ds(PAD - 1, nx)],
                lambda f: beside[j, side, f, pl.ds(PAD + 1, nx)],
                lambda f: yin[j, side, f],
                lambda f: rows[j, side, f],
                lambda f: zside[lax.rem(j, 2), side, f],
                lambda t: ghost_y[side, 1, t],
                lambda t: ghost_y[side, 2, t],
                lambda f: past[lax.rem(k, 2), 1, side, f],
            )
            for f in range(fields):
                past[lax.rem(k, 2), 1, side, f] = vector[f]
            found = precondition(
                lambda t: ghost_inv[1, side, t], lambda t: ghost_y[side, 1, t], vector
            )
            for f in range(fields):
                beside[k, side, f, own] = found[f]
            scatter(k, side, lambda f: found[f])
            packs = aside(k, side, found, packs)
        send_z(k, 1, packs, k < ITERS - 1)

    def x_given():
        packs = (blank, blank)
        for side in range(2):
            edge = nx + 1 if side else 0
            arrive(("x0", side), search.at[0, :, edge, own], along(0, side))
            found = [search[0, f, edge, own] for f in range(fields)]
            packs = across(0, side, edge, found, packs)
        send_z(0, 2, packs)

    def x_ghosts(k):
        packs = (blank, blank)
        j = k - 1
        take_x(j)
        take_z(j, 2)
        for side in range(2):
            edge, inner = (0, 1) if side == 0 else (nx + 1, nx)
            for f in range(fields):
                search[j, f, edge, PAD - 1 : PAD, :] = cin[j, side, 0, f : f + 1, :]
                search[j, f, edge, PAD + ny : PAD + ny + 1, :] = cin[j, side, 1, f : f + 1, :]
            vector = advance(
                j, 2, side * fields,
                lambda f: search[j, f, edge, own],
                lambda f: search[j, f, edge, pl.ds(PAD - 1, ny)],
                lambda f: search[j, f, edge, pl.ds(PAD + 1, ny)],
                lambda f: xin[j, side, f],
                lambda f: search[j, f, inner, own],
                lambda f: zsum[lax.rem(j, 2), f, edge],
                lambda t: ghost_x[side, 1, t],
                lambda t: ghost_x[side, 2, t],
                lambda f: past[lax.rem(k, 2), 0, side, f],
            )
            for f in range(fields):
                past[lax.rem(k, 2), 0, side, f] = vector[f]
            found = precondition(
                lambda t: ghost_inv[0, side, t], lambda t: ghost_x[side, 1, t], vector
            )
            for f in range(fields):
                search[k, f, edge, own] = found[f]
            packs = across(k, side, edge, found, packs)
        send_z(k, 2, packs, k < ITERS - 1)

    def dots(k):
        def group(g, carry):
            def step(place, accs):
                sums = [[] for _ in range(GROUP)]
                for x in range(SPAN):
                    x = place * SPAN + x
                    mine = [basis[k + 1, f, x, plane] for f in range(fields)]
                    for i in range(GROUP):
                        terms = [mine[f] * basis[g * GROUP + i + 1, f, x, plane] for f in range(fields)]
                        while len(terms) > 1:
                            terms = [a + b for a, b in zip(terms[::2], terms[1::2])]
                        sums[i].append(terms[0])
                return tuple(acc + sum(more) for acc, more in zip(accs, sums))

            accs = lax.fori_loop(0, nx // SPAN, step, (blank,) * GROUP)
            for i in range(GROUP):
                row = gram_row(g * GROUP + i, k)
                gram[pl.ds(row, 1), :] = jnp.sum(accs[i], axis=0, keepdims=True)
            return carry

        lax.fori_loop(0, lax.div(k, GROUP) + 1, group, 0)

    for load in loads:
        load.wait()

    def invert(x, carry):
        for t in range(levels):
            inv[t, x] = 1.0 / (time_rate + 6.0 + coef[0, t, x])
            for which in range(3):
                item = coef[which, t, x]
                given[0, which, t, pl.ds(x, 1), :] = item[ny - 1 : ny, :]
                given[1, which, t, pl.ds(x, 1), :] = item[0:1, :]
        return carry

    lax.fori_loop(0, nx, invert, 0)
    def first(planes, packs):
        founds = [
            precondition(
                lambda t: inv[t, x], lambda t: weight[t, x],
                [basis[1, f, x, plane] for f in range(fields)],
            )
            for x, _ in planes
        ]
        return spread(0, planes, founds, packs)

    def sweep(body, packs, low):
        return lax.fori_loop(
            0, (nx - 2 * low) // PLANES,
            lambda step, packs: body(
                [(low + step * PLANES + place, None) for place in range(PLANES)], packs
            ),
            packs,
        )

    pl.semaphore_wait(barrier, total - 1)
    for side in range(2):
        start(("gx", side), coef.at[:, :, nx - 1 if side == 0 else 0], ghost_x.at[side],
              along(0, side))
    for side in range(2):
        start(("gy", side), given.at[side], ghost_y.at[side], along(1, side))
    from_lane = lax.broadcasted_iota(jnp.int32, (2 * nz, 2 * nz), 0) & (nz - 1)
    to_lane = lax.broadcasted_iota(jnp.int32, (2 * nz, 2 * nz), 1)
    for odd in range(2):
        beside_lane = jnp.logical_or(from_lane - to_lane == 1, to_lane - from_lane == 1)
        last_lane = jnp.logical_and((to_lane & 1) == odd, from_lane == nz - 1)
        first_lane = jnp.logical_and((to_lane & 1) != odd, from_lane == 0)
        taken = jnp.where(
            to_lane < nz, beside_lane.astype(jnp.int32),
            jnp.logical_or(last_lane, first_lane).astype(jnp.int32),
        )
        mixer[odd] = taken.astype(jnp.float32).astype(jnp.bfloat16)
    ends = [(0, 1), (nx - 1, 0)]
    packs = first(ends, (blank, blank))
    packs = first([(1, None), (nx - 2, None)], packs)
    packs = sweep(first, packs, 2)
    for side in range(2):
        start(("x0", side), search.at[0, :, nx if side == 0 else 1, own],
              search.at[0, :, nx + 1 if side else 0, own], along(0, side))
    for side in range(2):
        start(("y0", side), rows.at[0, 1 - side], beside.at[0, side, :, own], along(1, side))
    send_z(0, 0, packs)
    send_c(0)
    send_x(0)
    send_y(0)
    dots(0)
    y_given()

    def iterate(k, carry):
        more = k < ITERS - 2

        @pl.when(k > 0)
        def _():
            y_ghosts(k)

        take_z(k, 0)
        body = functools.partial(own_planes, k)
        packs = body([(1, None), (nx - 2, None)], (blank, blank))
        send_x(k + 1, more)
        packs = sweep(body, packs, 2)

        @pl.when(k == 0)
        def _():
            x_given()

        @pl.when(k > 0)
        def _():
            x_ghosts(k)

        packs = body(ends, packs)
        send_z(k + 1, 0, packs, k < ITERS - 1)
        send_c(k + 1, more)
        send_y(k + 1, more)
        dots(k + 1)
        return carry

    lax.fori_loop(0, ITERS, iterate, 0)

    def settle(k, carry):
        more = k < ITERS - 1
        for side in range(2):
            drain(("x", k, side), xin.at[k, side], along(0, side), more)
            drain(("y", k, side), yin.at[k, side], along(1, side), more)
            for cy in range(2):
                drain(("c", k, side, cy), cin.at[k, side, cy], [1 - 2 * side, 1 - 2 * cy, 0], more)
            for kind in range(3):
                drain(("z", k, kind, side), zin.at[k, kind, side], along(2, side),
                      None if kind == 0 else more)
        return carry

    lax.fori_loop(0, ITERS, settle, 0)
    for side in range(2):
        drain(("x0", side), search.at[0, :, 0, own], along(0, side))
        drain(("y0", side), beside.at[0, side, :, own], along(1, side))
        drain(("gx", side), ghost_x.at[side], along(0, side))
        drain(("gy", side), ghost_y.at[side], along(1, side))

    local = jnp.sum(gram[...].T, axis=0, keepdims=True)
    gsend[...] = local
    gall[me] = local

    def spread(step, carry):
        pltpu.make_async_remote_copy(
            src_ref=gsend, dst_ref=gall.at[me], send_sem=gssem, recv_sem=grsem,
            device_id=ident((me + step) % total), device_id_type=pl.DeviceIdType.MESH,
        ).start()
        return carry

    lax.fori_loop(1, total, spread, 0)
    others = gall.at[pl.ds(0, total - 1)]
    pltpu.make_async_copy(others, others, grsem).wait()
    pltpu.make_async_copy(others, others, gssem).wait()
    whole = jnp.sum(gall[...], axis=0)
    splat[...] = jnp.broadcast_to(whole, splat.shape).T

    def entry(i, j):
        row = gram_row(i, j)
        return splat[row : row + 1, :]

    solved, worst = gram_solve(entry, ITERS)
    flag[...] = jnp.broadcast_to(worst, flag.shape)

    def combine(x, carry):
        for f in range(fields):
            item = solved[0] * search[0, f, x + 1, own]
            for k in range(1, ITERS):
                item = item + solved[k] * search[k, f, x + 1, own]
            ready[f, x] = item
        pltpu.make_async_copy(ready.at[:, x], out.at[:, x], osem).start()
        return carry

    lax.fori_loop(0, nx, combine, 0)
    pltpu.make_async_copy(ready, out, osem).wait()


def fused(sizes, residual, reaction, transport, congestion):
    levels, nx, ny, nz = reaction.shape
    fields = 2 * levels
    total = sizes[0] * sizes[1] * sizes[2]
    pairs = (ITERS + 1) ** 2
    assert (ITERS + 1) % GROUP == 0
    assert fields * nx <= nz and pairs <= nz and (nx - 4) % PLANES == 0 and nx == ny
    assert nz & (nz - 1) == 0
    f32 = jnp.float32
    hbm = pl.BlockSpec(memory_space=pl.ANY)
    vmem = pl.BlockSpec(memory_space=pltpu.VMEM)
    wide = ny + 3 * PAD
    copies = sum(width * cycle for _, width, cycle in CHANNELS.values()) + 2 * len(STARTS)
    out, flag = pl.pallas_call(
        functools.partial(kernel, levels, sizes),
        out_shape=(
            jax.ShapeDtypeStruct((fields, nx, ny, nz), f32),
            jax.ShapeDtypeStruct((8, nz), f32),
        ),
        in_specs=[hbm] * 4,
        out_specs=(hbm, vmem),
        scratch_shapes=[
            pltpu.VMEM((ITERS + 2, fields, nx + 1, ny + PAD, nz), f32),
            pltpu.VMEM((3, levels, nx, ny, nz), f32),
            pltpu.VMEM((levels, nx, ny, nz), f32),
            pltpu.VMEM((ITERS + 1, fields, nx + 2, wide, nz), f32),
            pltpu.VMEM((ITERS, 2, fields, wide, nz), f32),
            pltpu.VMEM((ITERS + 1, 2, fields, ny, nz), f32),
            pltpu.VMEM((ITERS + 1, 2, fields, nx, nz), f32),
            pltpu.VMEM((ITERS + 1, 2, fields, nx, nz), f32),
            pltpu.VMEM((ITERS + 1, 2, fields, nx, nz), f32),
            pltpu.VMEM((ITERS + 1, 2, 2, fields, nz), f32),
            pltpu.VMEM((ITERS + 1, 2, 2, fields, nz), f32),
            pltpu.VMEM((ITERS + 1, 3, 2, ny, nz), f32),
            pltpu.VMEM((ITERS + 1, 3, 2, ny, nz), f32),
            pltpu.VMEM((2, 3, levels, ny, nz), f32),
            pltpu.VMEM((2, 3, levels, nx, nz), f32),
            pltpu.VMEM((2, 2, levels, ny, nz), f32),
            pltpu.VMEM((2, 3, levels, nx, nz), f32),
            pltpu.VMEM((2, 2, 2, fields, ny, nz), f32),
            pltpu.VMEM((2, 2 * nz, 2 * nz), jnp.bfloat16),
            pltpu.VMEM((2, fields, nx + 2, ny, nz), f32),
            pltpu.VMEM((2, 2, fields, nx, nz), f32),
            pltpu.VMEM((nz, nz), f32),
            pltpu.VMEM((nz, nz), f32),
            pltpu.VMEM((1, nz), f32),
            pltpu.VMEM((total, 1, nz), f32),
            pltpu.VMEM((fields, nx, ny, nz), f32),
            pltpu.SemaphoreType.DMA((4,)),
            pltpu.SemaphoreType.DMA,
            pltpu.SemaphoreType.DMA((copies,)),
            pltpu.SemaphoreType.DMA,
            pltpu.SemaphoreType.DMA,
            pltpu.SemaphoreType.DMA,
        ],
        compiler_params=pltpu.CompilerParams(
            collective_id=0, has_side_effects=True, vmem_limit_bytes=60 * 1024 * 1024
        ),
        name="krylov",
    )(residual.reshape((fields, nx, ny, nz)), reaction, transport, congestion)
    return out.reshape(residual.shape), flag


def neighbours(field):
    total = 0.0
    for axis, dim in (("gx", 2), ("gy", 3), ("gz", 4)):
        count = lax.axis_size(axis)
        size = field.shape[dim]
        forward = [(i, i + 1) for i in range(count - 1)]
        backward = [(target, source) for source, target in forward]
        low = lax.ppermute(lax.slice_in_dim(field, size - 1, size, axis=dim), axis, forward)
        high = lax.ppermute(lax.slice_in_dim(field, 0, 1, axis=dim), axis, backward)
        below = jnp.concatenate([low, lax.slice_in_dim(field, 0, size - 1, axis=dim)], dim)
        above = jnp.concatenate([lax.slice_in_dim(field, 1, size, axis=dim), high], dim)
        total = total + below + above
    return total


def jacobian(vector, reaction, transport, congestion):
    lapped = 6.0 * vector - neighbours(vector)
    value_part, density_part = (vector[0], vector[1])
    later = jnp.concatenate([value_part[1:], jnp.zeros_like(value_part[:1])], 0)
    earlier = jnp.concatenate([jnp.zeros_like(density_part[:1]), density_part[:-1]], 0)
    first = (
        time_rate * (value_part - later)
        + lapped[0]
        + reaction * value_part
        - congestion * density_part
    )
    second = (
        time_rate * (density_part - earlier)
        + lapped[1]
        + reaction * density_part
        - transport * lapped[0]
    )
    return jnp.stack([first, second], 0)


def precondition(vector, reaction, transport):
    levels = vector.shape[1]
    diag = time_rate + 6.0 + reaction
    value_levels = [None] * levels
    carry = jnp.zeros_like(vector[0, 0])
    for level in range(levels - 1, -1, -1):
        carry = (vector[0, level] + time_rate * carry) / diag[level]
        value_levels[level] = carry
    density_levels = []
    carry = jnp.zeros_like(vector[1, 0])
    for level in range(levels):
        carry = (
            vector[1, level] + time_rate * carry + 6.0 * transport[level] * value_levels[level]
        ) / diag[level]
        density_levels.append(carry)
    return jnp.stack([jnp.stack(value_levels, 0), jnp.stack(density_levels, 0)], 0)


def arnoldi(residual, reaction, transport, congestion):
    dims = tuple(range(1, residual.ndim + 1))
    beta = jnp.sqrt(lax.psum(jnp.sum(residual * residual), AXES))
    basis = jnp.zeros((ITERS + 1,) + residual.shape, residual.dtype).at[0].set(residual / beta)
    heights = jnp.zeros((ITERS, ITERS + 1), residual.dtype)

    def step(c, state):
        basis, heights = state
        search = precondition(basis[c], reaction, transport)
        image = jacobian(search, reaction, transport, congestion)
        coeffs = lax.psum(jnp.sum(basis * image[None], axis=dims), AXES)
        image = image - jnp.sum(coeffs.reshape((-1,) + (1,) * residual.ndim) * basis, axis=0)
        height = jnp.sqrt(lax.psum(jnp.sum(image * image), AXES))
        basis = basis.at[c + 1].set(image / height)
        return basis, heights.at[c].set(coeffs.at[c + 1].set(height))

    basis, heights = lax.fori_loop(0, ITERS, step, (basis, heights))
    columns = [[heights[c, i] for i in range(c + 2)] for c in range(ITERS)]
    solved = least_squares(columns, beta, ITERS)
    mixed = sum(solved[c] * basis[c] for c in range(ITERS))
    return precondition(mixed, reaction, transport)


def body(sizes, residual_in, reaction, transport, congestion):
    update, flag = fused(sizes, residual_in, reaction, transport, congestion)
    return lax.cond(
        flag[0, 0] > PIVOT,
        lambda update, *rest: update,
        lambda update, *rest: arnoldi(*rest),
        update, residual_in, reaction, transport, congestion,
    )


def solution(mesh):
    placed = (
        P(None, None, "gx", "gy", "gz"),
        P(None, "gx", "gy", "gz"),
        P(None, "gx", "gy", "gz"),
        P(None, "gx", "gy", "gz"),
    )
    sizes = tuple(mesh.shape[axis] for axis in AXES)
    return jax.shard_map(
        functools.partial(body, sizes), mesh=mesh, in_specs=placed,
        out_specs=P(None, None, "gx", "gy", "gz"), check_vma=False,
    )
```
